128 devices in a mesh: dp: 8 (over y, x_lo), mp: 16 (over x_hi, z, core).
Axes of the slice: x: 4 (x_hi: 2, x_lo: 2; x = x_hi * 2 + x_lo), y: 4, z: 4, core: 2. Of those that a mesh axis runs over, the one named last changes fastest.
Arguments:
- tokens: bfloat16 [8, 2048, 5120], P('dp', 'mp'), may hold values from -6 to 6
- ln_gain: float32 [5120], replicated, may hold values from 0.1 to 1.9
- ln_bias: float32 [5120], replicated, may hold values from -3 to 3
- w_qkv: bfloat16 [5120, 3, 4096], P(None, None, 'mp'), may hold values from -0.15625 to 0.15625
- w_out: bfloat16 [4096, 5120], P('mp'), may hold values from -0.09375 to 0.09375
- grad_partial: bfloat16 [8, 4096, 5120], P('dp', 'mp'), may hold values from -6 to 6
Outputs:
- mixed: bfloat16 [8, 2048, 5120], P('dp', 'mp')
- grad_sum: float32 [4096, 5120], P('mp')
The draws below stay inside these ranges and needn't reach their ends.
All inputs are finite; a program needn't handle non-finite values.
Results may differ from the reference program's by a relative error of at most 0.014.
The reference program's roundings to bfloat16 on the way (of `normed`, `qkv`, `attn` and `context`) count: a program that leaves them out, or rounds other values in their place, can miss the bound.
Values may be sent and summed in bfloat16 or wider, within the bound.
A program may use at most 192 MiB of HBM per device.

```python
import jax
import jax.numpy as jnp
from jax import lax

D = 5120
HEAD = 128
HEADS = 32
SEQ = 128
IMG = 16
INNER = 4096
TOKENS = 2048
GROUPS = 8
N_MP = 16


def levels(key, shape, cuts, smallest, top_value):
    loudness = 1.0
    for dim, blocks in cuts:
        heights = jax.random.uniform(jax.random.fold_in(jax.random.fold_in(key, 6), dim), (blocks,), jnp.float32, smallest / len(cuts), top_value / len(cuts))
        loudness = loudness * jnp.repeat(jnp.exp(heights), shape[dim] // blocks).reshape((-1,) + (1,) * (len(shape) - 1 - dim))
    return loudness


def noise(rng, shape, scale, bound, shards=(), dtype=jnp.bfloat16):
    gain = levels(rng, shape, shards, -0.22, 0.18) if shards else 1.0
    drawn = jax.random.normal(rng, shape, jnp.float32) * scale * gain
    return jnp.minimum(jnp.maximum(drawn, -bound), bound).astype(dtype)


def setup_inputs(seed: int = 0) -> dict:
    streams_of = jax.random.split(jax.random.key(seed), 7)
    tokens = noise(streams_of[0], (GROUPS, TOKENS, D), 1.0, 6.0, ((0, 8), (1, 16)))
    ln_gain = jnp.clip(1.0 + 0.18 * jax.random.normal(streams_of[1], (D,), jnp.float32), 0.1, 1.9)
    ln_bias = noise(streams_of[2], (D,), 0.5, 3.0, (), jnp.float32)
    w_qkv = noise(streams_of[3], (D, 3, INNER), (D // 4) ** -0.5, 0.15625, ((2, 16),))
    w_out = noise(streams_of[4], (INNER, D), INNER ** -0.5, 0.09375, ((0, 16),))
    grad_partial = noise(streams_of[5], (GROUPS, INNER, D), 1.0, 6.0, ((0, 8), (1, 16)))
    return {"tokens": tokens, "ln_gain": ln_gain, "ln_bias": ln_bias, "w_qkv": w_qkv, "w_out": w_out, "grad_partial": grad_partial}


def layer_norm(rows, ln_gain, ln_bias):
    values = rows.astype(jnp.float32)
    center = lax.optimization_barrier(jnp.mean(values, axis=-1, keepdims=True))
    spread = lax.optimization_barrier(jnp.mean((values - center) * (values - center), axis=-1, keepdims=True))
    return ((values - center) * lax.rsqrt(spread + 1e-06) * ln_gain + ln_bias).astype(jnp.bfloat16)

def one_group(rows, ln_gain, ln_bias, w_qkv, w_out):
    normed = layer_norm(rows, ln_gain, ln_bias)
    qkv = jnp.dot(normed, w_qkv.reshape(D, 3 * INNER), preferred_element_type=jnp.float32).astype(jnp.bfloat16)
    query = qkv[:, :INNER].reshape(IMG, SEQ, HEADS, HEAD).astype(jnp.float32)
    keys = qkv[:, INNER:2 * INNER].reshape(IMG, SEQ, HEADS, HEAD).astype(jnp.float32)
    values = qkv[:, 2 * INNER:].reshape(IMG, SEQ, HEADS, HEAD).astype(jnp.float32)
    scores = jnp.einsum('bqhd,bkhd->bhqk', query, keys) * HEAD ** (-0.5)
    scaled = scores - lax.optimization_barrier(jnp.max(scores, axis=-1, keepdims=True))
    expsc = jnp.exp(scaled)
    attn = (expsc / lax.optimization_barrier(jnp.sum(expsc, axis=-1, keepdims=True))).astype(jnp.bfloat16)
    context = jnp.einsum('bhqk,bkhd->bqhd', attn.astype(jnp.float32), values).astype(jnp.bfloat16)
    context = context.reshape(TOKENS, INNER)
    width = INNER // N_MP

    def add_group(index, total):
        start = (index * width).astype(jnp.int32)
        cols = lax.dynamic_slice_in_dim(context, start, width, 1)
        wrows = lax.dynamic_slice_in_dim(w_out, start, width, 0)
        partial_sum = jnp.dot(cols, wrows, preferred_element_type=jnp.float32).astype(jnp.bfloat16)
        partial_sum = lax.optimization_barrier(partial_sum)
        return total + partial_sum.astype(jnp.float32)
    proj = lax.fori_loop(0, N_MP, add_group, jnp.zeros((TOKENS, D), jnp.float32))
    return (rows.astype(jnp.float32) + proj).astype(jnp.bfloat16)

def reference(tokens, ln_gain, ln_bias, w_qkv, w_out, grad_partial):
    mixed = lax.map(lambda rows: one_group(rows, ln_gain, ln_bias, w_qkv, w_out), tokens)
    grad_sum = lax.optimization_barrier(jnp.sum(grad_partial.astype(jnp.float32), axis=0))
    return (mixed, grad_sum)
```

```python
import jax
import jax.numpy as jnp
from jax import lax
from jax.experimental import pallas as pl
from jax.experimental.pallas import tpu as pltpu
from jax.sharding import PartitionSpec as P

HEAD = 128
SEQ = 128
D = 5120
NY = 4
NZ = 4
WIDTH = 256
HALF = SEQ // 2
QUART = SEQ // 4
GROWS = WIDTH // NY
MESH = pl.DeviceIdType.MESH
BF = jnp.bfloat16
F32 = jnp.float32


def attend(query, keys, values):
    scores = lax.dot_general(
        query, keys, (((1,), (1,)), ((), ())), preferred_element_type=F32
    ) * HEAD ** (-0.5)
    scaled = scores - jnp.max(scores, axis=-1, keepdims=True)
    expsc = jnp.exp(scaled)
    attn = (expsc / jnp.sum(expsc, axis=-1, keepdims=True)).astype(BF)
    return jnp.dot(attn, values, preferred_element_type=F32).astype(BF)


def kernel(
    tok_hbm, gain, bias, wq_hbm, wo_hbm, g_hbm,
    mixed_hbm, gsum_hbm,
    raw, T, WQ, WO, QKV, CTX, CTXR, PS, RB,
    GO, GR, GX, GXR, GT, GA, GF, OM,
    zs, zr, xs, xr, cs, cr, rss, rsr,
    wqs, wqr, wos, wor, gs, gr, loc, outs,
):
    dp = lax.axis_index("dp")
    mp = lax.axis_index("mp")
    y, xl = dp // 2, dp % 2
    xh, z, c = mp // 8, (mp // 2) % 4, mp % 2

    def dev(y, xl, xh, z, c):
        return (lax.rem(y + NY, NY) * 2 + xl, xh * 8 + lax.rem(z + NZ, NZ) * 2 + c)

    zdev = (dev(y, xl, xh, z + 1, c), dev(y, xl, xh, z - 1, c))
    x2 = dev(y, xl, 1 - xh, z, c)
    mate = dev(y, xl, xh, z, 1 - c)
    cross = dev(y, 1 - xl, 1 - xh, z, c)
    xlo = dev(y, 1 - xl, xh, z, c)
    ydev = [dev(y + k, xl, xh, z, c) for k in (1, 2, 3 - NY)]

    def local(src, dst, sem):
        copy = pltpu.make_async_copy(src, dst, sem)
        copy.start()
        return copy

    load_raw = local(tok_hbm, raw, loc.at[0])
    load_wq = [local(wq_hbm.at[j], WQ.at[c * 3 + j], loc.at[1 + j]) for j in range(3)]
    own_seg = pl.multiple_of((xh * 2 + c) * WIDTH, WIDTH)
    far_seg = pl.multiple_of(((1 - xh) * 2 + c) * WIDTH, WIDTH)
    load_wo = local(wo_hbm, WO.at[pl.ds(own_seg, WIDTH)], loc.at[4])
    my_rows = pl.ds(pl.multiple_of(y * GROWS, GROWS), GROWS)
    load_g = local(g_hbm.at[my_rows], GO, loc.at[5])

    barrier = pltpu.get_barrier_semaphore()
    peers = [*zdev, x2, mate, cross, xlo, *ydev]
    for peer in peers:
        pl.semaphore_signal(barrier, inc=1, device_id=peer, device_id_type=MESH)
    pl.semaphore_wait(barrier, len(peers))

    sent = []

    def send(src, dst, ssem, rsem, peer):
        copy = pltpu.make_async_remote_copy(
            src_ref=src, dst_ref=dst, send_sem=ssem, recv_sem=rsem,
            device_id=peer, device_id_type=MESH,
        )
        copy.start()
        sent.append(copy)
        return copy

    wo_cross = send(
        wo_hbm.at[my_rows], WO.at[pl.ds(own_seg + y * GROWS, GROWS)],
        wos.at[0], wor.at[0], cross,
    )
    wq_mate = [
        send(wq_hbm.at[j], WQ.at[c * 3 + j], wqs.at[j], wqr.at[j], mate) for j in range(3)
    ]
    wo_mate = send(wo_hbm, WO.at[pl.ds(own_seg, WIDTH)], wos.at[1], wor.at[1], mate)
    g_rs = []
    for k in range(3):
        rows = pl.ds(pl.multiple_of(lax.rem(y + k + 1, NY) * GROWS, GROWS), GROWS)
        g_rs.append(send(g_hbm.at[rows], GR.at[k], gs.at[k], gr.at[k], ydev[k]))

    def slot(col, zz):
        return col * NZ + lax.rem(zz + 2 * NZ, NZ)

    def quarter(h, q):
        return pl.ds(h * HALF + q * QUART, QUART)

    zcopy, xcopy = {}, {}

    def zsend(step, h, q, s):
        ref = T.at[s, quarter(h, q)]
        zcopy[step, h, q] = send(ref, ref, zs.at[h, step, q], zr.at[h, step, q], zdev[h])

    def xsend(step, h, q, s):
        ref = T.at[s, quarter(h, q)]
        xcopy[step, h, q] = send(ref, ref, xs.at[step, h, q], xr.at[step, h, q], x2)

    sign = (1, -1)
    own = slot(xh, z)

    load_raw.wait()
    for q in range(2):
        for h in range(2):
            @pl.loop(0, QUART // 16)
            def _(i, h=h, q=q):
                rows = pl.ds(pl.multiple_of(h * HALF + q * QUART + i * 16, 16), 16)
                values = raw[rows, :].astype(F32)
                center = jnp.mean(values, axis=-1, keepdims=True)
                spread = jnp.mean((values - center) * (values - center), axis=-1, keepdims=True)
                T[own, rows, :] = (
                    (values - center) * lax.rsqrt(spread + 1e-06) * gain[...] + bias[...]
                ).astype(BF)
            zsend(0, h, q, own)
            xsend(0, h, q, own)

    def project(s, base, count):
        @pl.loop(0, count)
        def _(j):
            QKV[base + j] = jnp.dot(T[s], WQ[base + j], preferred_element_type=F32).astype(BF)

    def attention(s):
        for cc in range(2):
            for h in range(2):
                cols = slice(h * HEAD, (h + 1) * HEAD)
                CTX[s, :, cc * WIDTH + h * HEAD:cc * WIDTH + (h + 1) * HEAD] = attend(
                    QKV[cc * 3, :, cols], QKV[cc * 3 + 1, :, cols], QKV[cc * 3 + 2, :, cols]
                )

    ccopy = {}

    def ctx_send(k):
        zz = lax.rem(z + k, NZ)
        ccopy[k] = send(CTX.at[slot(1 - xh, z + k)], CTXR.at[zz], cs.at[k], cr.at[k], x2)

    for copy in load_wq:
        copy.wait()
    project(own, c * 3, 3)
    for h in range(2):
        zcopy[0, h, 0].wait_recv()
        zsend(1, h, 0, slot(xh, z - sign[h]))
    for copy in wq_mate:
        copy.wait_recv()
    project(own, (1 - c) * 3, 3)
    attention(own)
    for h in range(2):
        zcopy[0, h, 1].wait_recv()
        zsend(1, h, 1, slot(xh, z - sign[h]))

    wo_cross.wait_recv()
    far_rows = WO.at[pl.ds(far_seg + y * GROWS, GROWS)]
    wo_y = [send(far_rows, far_rows, wos.at[2 + k], wor.at[2 + k], ydev[k]) for k in range(3)]
    wo_fwd = [send(far_rows, far_rows, wos.at[5], wor.at[5], mate)]

    for q in range(2):
        for h in range(2):
            zcopy[1, h, q].wait_recv()
            zsend(2, h, q, slot(xh, z + 2))
            xsend(1, h, q, slot(xh, z + 2))
    for q in range(2):
        for h in range(2):
            xcopy[0, h, q].wait_recv()
            zsend(3, h, q, slot(1 - xh, z))

    @pl.loop(0, 2)
    def _(i):
        s = jnp.where(i == 0, slot(1 - xh, z), slot(xh, z + 2))
        project(s, 0, 6)
        attention(s)
    ctx_send(0)

    for q in range(2):
        for h in range(2):
            zcopy[2, h, q].wait_recv()
    for h in range(2):
        xcopy[1, h, 0].wait_recv()
        zsend(4, h, 0, slot(1 - xh, z + 2))

    @pl.loop(0, 2)
    def _(i):
        s = slot(xh, z + 1 + 2 * i)
        project(s, 0, 6)
        attention(s)

    for h in range(2):
        xcopy[1, h, 1].wait_recv()
        zsend(4, h, 1, slot(1 - xh, z + 2))

    def by_rows(count, fn):
        @pl.loop(0, count // 16)
        def _(i):
            fn(pl.ds(pl.multiple_of(i * 16, 16), 16))

    load_g.wait()
    for copy in g_rs:
        copy.wait_recv()

    def sum4(rows):
        GX[rows, :] = (
            (GO[rows, :].astype(F32) + GR[0, rows, :].astype(F32))
            + (GR[1, rows, :].astype(F32) + GR[2, rows, :].astype(F32))
        ).astype(BF)
    by_rows(GROWS, sum4)
    g_x = send(GX, GXR, gs.at[3], gr.at[3], xlo)

    for k in range(3):
        wo_y[k].wait_recv()
        rows = WO.at[pl.ds(far_seg + lax.rem(y + NY - k - 1, NY) * GROWS, GROWS)]
        wo_fwd.append(send(rows, rows, wos.at[6 + k], wor.at[6 + k], mate))

    project(slot(1 - xh, z + 2), 0, 6)
    attention(slot(1 - xh, z + 2))
    ctx_send(2)

    load_wo.wait()
    wo_mate.wait_recv()
    for copy in wo_fwd:
        copy.wait_recv()

    def out_project(k):
        zz = lax.rem(z + k, NZ)
        near = pl.ds(pl.multiple_of(xh * 2 * WIDTH, WIDTH), 2 * WIDTH)
        far = pl.ds(pl.multiple_of((1 - xh) * 2 * WIDTH, WIDTH), 2 * WIDTH)

        @pl.loop(0, D // 512)
        def _(j):
            cols = pl.ds(pl.multiple_of(j * 512, 512), 512)
            PS[zz, :, cols] = (
                jnp.dot(CTX[slot(xh, zz)], WO[near, cols], preferred_element_type=F32)
                + jnp.dot(CTXR[zz], WO[far, cols], preferred_element_type=F32)
            ).astype(BF)

    ccopy[0].wait_recv()
    out_project(0)

    g_x.wait_recv()

    def sum2(rows):
        GT[rows, :] = (GX[rows, :].astype(F32) + GXR[rows, :].astype(F32)).astype(BF)
    by_rows(GROWS, sum2)
    g_ag = [send(GT, GA.at[k], gs.at[4 + k], gr.at[4 + k], ydev[k]) for k in range(3)]

    ccopy[2].wait_recv()
    out_project(2)

    rcopy = {}

    def rsend(kind, q, image, h, to):
        ref = PS.at[lax.rem(image + 2 * NZ, NZ), quarter(h, q)]
        rcopy[kind, q] = send(
            ref, RB.at[kind, pl.ds(q * QUART, QUART)],
            rss.at[kind, q], rsr.at[kind, q], zdev[to],
        )

    for q in range(2):
        rsend(0, q, z + 2, 0, 1)
        rsend(1, q, z + 2, 1, 0)

    for q in range(2):
        for h in range(2):
            zcopy[3, h, q].wait_recv()
            zcopy[4, h, q].wait_recv()
    for k in (1, 3):
        project(slot(1 - xh, z + k), 0, 6)
        attention(slot(1 - xh, z + k))
        ctx_send(k)
    ccopy[1].wait_recv()
    out_project(1)
    for q in range(2):
        rsend(4, q, z + 1, 0, 0)
    ccopy[3].wait_recv()
    out_project(3)
    for q in range(2):
        rsend(5, q, z - 1, 1, 1)

    for q in range(2):
        for h in range(2):
            image = lax.rem(z - sign[h] + NZ, NZ)
            rcopy[h, q].wait_recv()

            @pl.loop(0, QUART // 16)
            def _(i, h=h, q=q, image=image):
                at = pl.multiple_of(q * QUART + i * 16, 16)
                rows = pl.ds(h * HALF + at, 16)
                PS[image, rows, :] = (
                    PS[image, rows, :].astype(F32) + RB[h, pl.ds(at, 16), :].astype(F32)
                ).astype(BF)
            rsend(2 + h, q, z - sign[h], h, 1 - h)

    written = []
    for k in range(4):
        if k:
            g_ag[k - 1].wait_recv()
        if k >= 2:
            written[k - 2].wait()

        def widen(rows, k=k):
            part = GT[rows, :] if k == 0 else GA[k - 1, rows, :]
            GF[k % 2, rows, :] = part.astype(F32)
        by_rows(GROWS, widen)
        rows = pl.ds(pl.multiple_of(lax.rem(y + NY - k, NY) * GROWS, GROWS), GROWS)
        written.append(local(GF.at[k % 2], gsum_hbm.at[rows], outs.at[k]))

    for q in range(2):
        for h in range(2):
            rcopy[4 + h, q].wait_recv()
            rcopy[2 + h, q].wait_recv()

            @pl.loop(0, QUART // 16)
            def _(i, h=h, q=q):
                at = pl.multiple_of(q * QUART + i * 16, 16)
                rows = pl.ds(h * HALF + at, 16)
                part = pl.ds(at, 16)
                proj = PS[z, rows, :].astype(F32) + (
                    RB[2 + h, part, :].astype(F32) + RB[4 + h, part, :].astype(F32)
                )
                OM[rows, :] = (raw[rows, :].astype(F32) + proj).astype(BF)
            written.append(
                local(OM.at[quarter(h, q)], mixed_hbm.at[quarter(h, q)], outs.at[4 + h * 2 + q])
            )
    for copy in written[2:]:
        copy.wait()
    for copy in sent:
        copy.wait_send()


def body(tokens, ln_gain, ln_bias, w_qkv, w_out, grad_partial):
    dma = pltpu.SemaphoreType.DMA
    any_spec = pl.BlockSpec(memory_space=pl.ANY)
    vmem = pl.BlockSpec(memory_space=pltpu.VMEM)
    mixed, grad_sum = pl.pallas_call(
        kernel,
        out_shape=(
            jax.ShapeDtypeStruct((SEQ, D), BF),
            jax.ShapeDtypeStruct((WIDTH, D), F32),
        ),
        in_specs=[any_spec, vmem, vmem, any_spec, any_spec, any_spec],
        out_specs=(any_spec, any_spec),
        scratch_shapes=[
            pltpu.VMEM((SEQ, D), BF),
            pltpu.VMEM((2 * NZ, SEQ, D), BF),
            pltpu.VMEM((6, D, WIDTH), BF),
            pltpu.VMEM((4 * WIDTH, D), BF),
            pltpu.VMEM((6, SEQ, WIDTH), BF),
            pltpu.VMEM((2 * NZ, SEQ, 2 * WIDTH), BF),
            pltpu.VMEM((NZ, SEQ, 2 * WIDTH), BF),
            pltpu.VMEM((NZ, SEQ, D), BF),
            pltpu.VMEM((6, HALF, D), BF),
            pltpu.VMEM((GROWS, D), BF),
            pltpu.VMEM((3, GROWS, D), BF),
            pltpu.VMEM((GROWS, D), BF),
            pltpu.VMEM((GROWS, D), BF),
            pltpu.VMEM((GROWS, D), BF),
            pltpu.VMEM((3, GROWS, D), BF),
            pltpu.VMEM((2, GROWS, D), F32),
            pltpu.VMEM((SEQ, D), BF),
            dma((2, 5, 2)), dma((2, 5, 2)),
            dma((2, 2, 2)), dma((2, 2, 2)),
            dma((4,)), dma((4,)),
            dma((6, 2)), dma((6, 2)),
            dma((3,)), dma((3,)),
            dma((9,)), dma((9,)),
            dma((7,)), dma((7,)),
            dma((6,)), dma((8,)),
        ],
        compiler_params=pltpu.CompilerParams(
            collective_id=0, has_side_effects=True, vmem_limit_bytes=67043328
        ),
    )(
        tokens[0], ln_gain[None], ln_bias[None],
        jnp.transpose(w_qkv, (1, 0, 2)), w_out, grad_partial[0],
    )
    return (mixed[None], grad_sum)


def solution(mesh):
    placed = (
        P("dp", "mp", None),
        P(),
        P(),
        P(None, None, "mp"),
        P("mp", None),
        P("dp", "mp", None),
    )
    return jax.shard_map(
        body,
        mesh=mesh,
        in_specs=placed,
        out_specs=(P("dp", "mp", None), P("mp", None)),
        check_vma=False,
    )
```

```python
import jax
import jax.numpy as jnp
from jax import lax
from jax.experimental import pallas as pl
from jax.experimental.pallas import tpu as pltpu
from jax.sharding import PartitionSpec as P

HEAD = 128
SEQ = 128
D = 5120
NY = 4
NZ = 4
WIDTH = 256
HALF = SEQ // 2
QUART = SEQ // 4
GROWS = WIDTH // NY
MESH = pl.DeviceIdType.MESH
BF = jnp.bfloat16
F32 = jnp.float32


def attend(query, keys, values):
    scores = lax.dot_general(
        query, keys, (((1,), (1,)), ((), ())), preferred_element_type=F32
    ) * HEAD ** (-0.5)
    scaled = scores - jnp.max(scores, axis=-1, keepdims=True)
    expsc = jnp.exp(scaled)
    attn = (expsc / jnp.sum(expsc, axis=-1, keepdims=True)).astype(BF)
    return jnp.dot(attn, values, preferred_element_type=F32).astype(BF)


def kernel(
    tok_hbm, gain, bias, wq_hbm, wo_hbm, g_hbm,
    mixed_hbm, gsum_hbm,
    raw, T, WQ, WO, QKV, CTX, CTXR, PS, RB,
    GO, GR, GX, GXR, GT, GA, OM,
    zs, zr, xs, xr, cs, cr, rss, rsr,
    wqs, wqr, wos, wor, gs, gr, loc, outs,
):
    dp = lax.axis_index("dp")
    mp = lax.axis_index("mp")
    y, xl = dp // 2, dp % 2
    xh, z, c = mp // 8, (mp // 2) % 4, mp % 2

    def dev(y, xl, xh, z, c):
        return (lax.rem(y + NY, NY) * 2 + xl, xh * 8 + lax.rem(z + NZ, NZ) * 2 + c)

    zdev = (dev(y, xl, xh, z + 1, c), dev(y, xl, xh, z - 1, c))
    x2 = dev(y, xl, 1 - xh, z, c)
    mate = dev(y, xl, xh, z, 1 - c)
    cross = dev(y, 1 - xl, 1 - xh, z, c)
    xlo = dev(y, 1 - xl, xh, z, c)
    ydev = [dev(y + k, xl, xh, z, c) for k in (1, 2, 3 - NY)]

    def local(src, dst, sem):
        copy = pltpu.make_async_copy(src, dst, sem)
        copy.start()
        return copy

    load_raw = local(tok_hbm, raw, loc.at[0])
    load_wq = [local(wq_hbm.at[j], WQ.at[c * 3 + j], loc.at[1 + j]) for j in range(3)]
    own_seg = pl.multiple_of((xh * 2 + c) * WIDTH, WIDTH)
    far_seg = pl.multiple_of(((1 - xh) * 2 + c) * WIDTH, WIDTH)
    load_wo = local(wo_hbm, WO.at[pl.ds(own_seg, WIDTH)], loc.at[4])
    my_rows = pl.ds(pl.multiple_of(y * GROWS, GROWS), GROWS)
    load_g = local(g_hbm.at[my_rows], GO, loc.at[5])

    barrier = pltpu.get_barrier_semaphore()
    peers = [*zdev, x2, mate, cross, xlo, *ydev]
    for peer in peers:
        pl.semaphore_signal(barrier, inc=1, device_id=peer, device_id_type=MESH)

    def slot(col, zz):
        return col * NZ + lax.rem(zz + 2 * NZ, NZ)

    own = slot(xh, z)
    load_raw.wait()

    @pl.loop(0, SEQ // 16)
    def _(i):
        rows = pl.ds(pl.multiple_of(i * 16, 16), 16)
        values = raw[rows, :].astype(F32)
        center = jnp.mean(values, axis=-1, keepdims=True)
        spread = jnp.mean((values - center) * (values - center), axis=-1, keepdims=True)
        T[own, rows, :] = (
            (values - center) * lax.rsqrt(spread + 1e-06) * gain[...] + bias[...]
        ).astype(BF)

    pl.semaphore_wait(barrier, len(peers))

    sent = []

    def send(src, dst, ssem, rsem, peer):
        copy = pltpu.make_async_remote_copy(
            src_ref=src, dst_ref=dst, send_sem=ssem, recv_sem=rsem,
            device_id=peer, device_id_type=MESH,
        )
        copy.start()
        sent.append(copy)
        return copy

    def part(seg, yy):
        return pl.ds(pl.multiple_of(seg + yy * GROWS, GROWS), GROWS)

    wo_cross = send(
        wo_hbm.at[part(0, y)], WO.at[part(own_seg, y)], wos.at[0], wor.at[0], cross
    )

    def quarter(h, q):
        return pl.ds(h * HALF + q * QUART, QUART)

    zcopy, xcopy = {}, {}

    def zsend(step, h, q, s):
        ref = T.at[s, quarter(h, q)]
        zcopy[step, h, q] = send(ref, ref, zs.at[step, h, q], zr.at[step, h, q], zdev[h])

    def xsend(step, h, q, s):
        ref = T.at[s, quarter(h, q)]
        xcopy[step, h] = send(ref, ref, xs.at[step, h], xr.at[step, h], x2)

    sign = (1, -1)
    for q in range(2):
        for h in range(2):
            zsend(0, h, q, own)

    wq_mate = [
        send(wq_hbm.at[j], WQ.at[c * 3 + j], wqs.at[j], wqr.at[j], mate) for j in range(3)
    ]
    wo_mate = send(wo_hbm, WO.at[pl.ds(own_seg, WIDTH)], wos.at[1], wor.at[1], mate)
    g_rs = []
    for k in range(3):
        rows = pl.ds(pl.multiple_of(lax.rem(y + k + 1, NY) * GROWS, GROWS), GROWS)
        g_rs.append(send(g_hbm.at[rows], GR.at[k], gs.at[k], gr.at[k], ydev[k]))

    def project(s, base, count):
        @pl.loop(0, count)
        def _(j):
            QKV[base + j] = jnp.dot(T[s], WQ[base + j], preferred_element_type=F32).astype(BF)

    def attention(s):
        for cc in range(2):
            for h in range(2):
                cols = slice(h * HEAD, (h + 1) * HEAD)
                CTX[s, :, cc * WIDTH + h * HEAD:cc * WIDTH + (h + 1) * HEAD] = attend(
                    QKV[cc * 3, :, cols], QKV[cc * 3 + 1, :, cols], QKV[cc * 3 + 2, :, cols]
                )

    ccopy = {}

    def ctx_send(k):
        zz = lax.rem(z + k, NZ)
        ccopy[k] = send(CTX.at[slot(1 - xh, z + k)], CTXR.at[zz], cs.at[k], cr.at[k], x2)

    def by_rows(count, fn):
        @pl.loop(0, count // 16)
        def _(i):
            fn(pl.ds(pl.multiple_of(i * 16, 16), 16))

    for copy in load_wq:
        copy.wait()
    project(own, c * 3, 3)
    for h in range(2):
        zcopy[0, h, 0].wait_recv()
        zsend(1, h, 0, slot(xh, z - sign[h]))
    for copy in wq_mate:
        copy.wait_recv()
    project(own, (1 - c) * 3, 3)
    attention(own)

    wo_cross.wait_recv()
    for h in range(2):
        xsend(0, h, 1, own)
    rows = WO.at[part(far_seg, y)]
    wo_y = [send(rows, rows, wos.at[2 + k], wor.at[2 + k], ydev[k]) for k in range(3)]
    wo_fwd = [send(rows, rows, wos.at[5], wor.at[5], mate)]

    for h in range(2):
        zcopy[0, h, 1].wait_recv()
        zsend(1, h, 1, slot(xh, z - sign[h]))
    for h in range(2):
        zcopy[1, h, 0].wait_recv()
        zsend(2, h, 0, slot(xh, z + 2))
        xsend(1, h, 0, slot(xh, z + 2))
    for h in range(2):
        xsend(2, h, 0, slot(xh, z - sign[h]))
    for h in range(2):
        zcopy[1, h, 1].wait_recv()
        xcopy[0, h].wait_recv()
        zsend(3, h, 1, slot(1 - xh, z))
        zsend(2, h, 1, slot(xh, z + 2))
    project(slot(xh, z + 2), 0, 6)
    attention(slot(xh, z + 2))

    for h in range(2):
        zcopy[3, h, 1].wait_recv()
        zsend(4, h, 1, slot(1 - xh, z - sign[h]))
    for h in range(2):
        xcopy[1, h].wait_recv()
        zsend(3, h, 0, slot(1 - xh, z + 2))
    for q in range(2):
        for h in range(2):
            zcopy[2, h, q].wait_recv()
    project(slot(xh, z + 1), 0, 6)
    attention(slot(xh, z + 1))

    load_g.wait()
    for copy in g_rs:
        copy.wait_recv()

    def sum4(rows):
        GX[rows, :] = (
            (GO[rows, :].astype(F32) + GR[0, rows, :].astype(F32))
            + (GR[1, rows, :].astype(F32) + GR[2, rows, :].astype(F32))
        ).astype(BF)
    by_rows(GROWS, sum4)
    g_x = send(GX, GXR, gs.at[3], gr.at[3], xlo)

    for h in range(2):
        zcopy[4, h, 1].wait_recv()
        zsend(5, h, 1, slot(1 - xh, z + 2))
    project(slot(1 - xh, z + 2), 0, 6)
    attention(slot(1 - xh, z + 2))
    ctx_send(2)

    for k in range(3):
        wo_y[k].wait_recv()
        rows = WO.at[part(far_seg, lax.rem(y + NY - k - 1, NY))]
        wo_fwd.append(send(rows, rows, wos.at[6 + k], wor.at[6 + k], mate))
    project(slot(xh, z + 3), 0, 6)
    attention(slot(xh, z + 3))

    load_wo.wait()
    wo_mate.wait_recv()
    for copy in wo_fwd:
        copy.wait_recv()

    def out_project(k):
        zz = lax.rem(z + k, NZ)
        near = pl.ds(pl.multiple_of(xh * 2 * WIDTH, WIDTH), 2 * WIDTH)
        far = pl.ds(pl.multiple_of((1 - xh) * 2 * WIDTH, WIDTH), 2 * WIDTH)

        @pl.loop(0, D // 512)
        def _(j):
            cols = pl.ds(pl.multiple_of(j * 512, 512), 512)
            PS[zz, :, cols] = (
                jnp.dot(CTX[slot(xh, zz)], WO[near, cols], preferred_element_type=F32)
                + jnp.dot(CTXR[zz], WO[far, cols], preferred_element_type=F32)
            ).astype(BF)

    ccopy[2].wait_recv()
    out_project(2)

    rcopy = {}

    def rsend(kind, q, image, h, to):
        ref = PS.at[lax.rem(image + 2 * NZ, NZ), quarter(h, q)]
        rcopy[kind, q] = send(
            ref, RB.at[kind, pl.ds(q * QUART, QUART)],
            rss.at[kind, q], rsr.at[kind, q], zdev[to],
        )

    for q in range(2):
        rsend(0, q, z + 2, 0, 1)
        rsend(1, q, z + 2, 1, 0)

    for h in range(2):
        zcopy[3, h, 0].wait_recv()
        zcopy[5, h, 1].wait_recv()
        xcopy[2, h].wait_recv()
    for k in (1, 3):
        project(slot(1 - xh, z + k), 0, 6)
        attention(slot(1 - xh, z + k))
        ctx_send(k)
    for h in range(2):
        xsend(3, h, 0, own)

    g_x.wait_recv()

    def sum2(rows):
        GT[rows, :] = (GX[rows, :].astype(F32) + GXR[rows, :].astype(F32)).astype(BF)
    by_rows(GROWS, sum2)
    g_ag = [send(GT, GA.at[k], gs.at[4 + k], gr.at[4 + k], ydev[k]) for k in range(3)]

    ccopy[1].wait_recv()
    out_project(1)
    for q in range(2):
        rsend(4, q, z + 1, 0, 0)
    ccopy[3].wait_recv()
    out_project(3)
    for q in range(2):
        rsend(5, q, z - 1, 1, 1)

    for q in range(2):
        for h in range(2):
            image = lax.rem(z - sign[h] + NZ, NZ)
            rcopy[h, q].wait_recv()

            @pl.loop(0, QUART // 16)
            def _(i, h=h, q=q, image=image):
                at = pl.multiple_of(q * QUART + i * 16, 16)
                rows = pl.ds(h * HALF + at, 16)
                PS[image, rows, :] = (
                    PS[image, rows, :].astype(F32) + RB[h, pl.ds(at, 16), :].astype(F32)
                ).astype(BF)
            rsend(2 + h, q, z - sign[h], h, 1 - h)

    for h in range(2):
        xcopy[3, h].wait_recv()
    project(slot(1 - xh, z), 0, 6)
    attention(slot(1 - xh, z))
    ctx_send(0)
    ccopy[0].wait_recv()
    out_project(0)

    written = [local(GT, gsum_hbm.at[my_rows], outs.at[0])]
    for k in range(3):
        g_ag[k].wait_recv()
        rows = pl.ds(pl.multiple_of(lax.rem(y + NY - k - 1, NY) * GROWS, GROWS), GROWS)
        written.append(local(GA.at[k], gsum_hbm.at[rows], outs.at[1 + k]))

    for q in range(2):
        for h in range(2):
            rcopy[4 + h, q].wait_recv()
            rcopy[2 + h, q].wait_recv()

            @pl.loop(0, QUART // 16)
            def _(i, h=h, q=q):
                at = pl.multiple_of(q * QUART + i * 16, 16)
                rows = pl.ds(h * HALF + at, 16)
                part = pl.ds(at, 16)
                proj = PS[z, rows, :].astype(F32) + (
                    RB[2 + h, part, :].astype(F32) + RB[4 + h, part, :].astype(F32)
                )
                OM[rows, :] = (raw[rows, :].astype(F32) + proj).astype(BF)
            written.append(
                local(OM.at[quarter(h, q)], mixed_hbm.at[quarter(h, q)], outs.at[4 + h * 2 + q])
            )
    for copy in written:
        copy.wait()
    for copy in sent:
        copy.wait_send()


NG = 8
NM = 2


def finish(mixed_in, grad_in, mixed_out, grad_out, held, narrow, wide, isem, osem):
    def chunk(n, i, total):
        return pl.ds(i * (total // n), total // n)

    def copy(src, dst, sem):
        made = pltpu.make_async_copy(src, dst, sem)
        made.start()
        return made

    grads = [chunk(NG, i, WIDTH) for i in range(NG)]
    rows = [chunk(NM, i, SEQ) for i in range(NM)]
    came = [copy(grad_in.at[r], narrow.at[r], isem.at[i]) for i, r in enumerate(grads)]
    came += [copy(mixed_in.at[r], held.at[r], isem.at[NG + i]) for i, r in enumerate(rows)]
    left = []
    for i, r in enumerate(grads):
        came[i].wait()

        @pl.loop(0, WIDTH // NG // 16)
        def _(j, i=i):
            at = pl.ds(pl.multiple_of(i * (WIDTH // NG) + j * 16, 16), 16)
            wide[at, :] = narrow[at, :].astype(F32)
        left.append(copy(wide.at[r], grad_out.at[r], osem.at[i]))
    for i, r in enumerate(rows):
        came[NG + i].wait()
        left.append(copy(held.at[r], mixed_out.at[r], osem.at[NG + i]))
    for made in left:
        made.wait()


def body(tokens, ln_gain, ln_bias, w_qkv, w_out, grad_partial):
    dma = pltpu.SemaphoreType.DMA
    any_spec = pl.BlockSpec(memory_space=pl.ANY)
    vmem = pl.BlockSpec(memory_space=pltpu.VMEM)
    mixed, grad_sum = pl.pallas_call(
        kernel,
        out_shape=(
            jax.ShapeDtypeStruct((SEQ, D), BF),
            jax.ShapeDtypeStruct((WIDTH, D), BF),
        ),
        in_specs=[any_spec, vmem, vmem, any_spec, any_spec, any_spec],
        out_specs=(any_spec, any_spec),
        scratch_shapes=[
            pltpu.VMEM((SEQ, D), BF),
            pltpu.VMEM((2 * NZ, SEQ, D), BF),
            pltpu.VMEM((6, D, WIDTH), BF),
            pltpu.VMEM((4 * WIDTH, D), BF),
            pltpu.VMEM((6, SEQ, WIDTH), BF),
            pltpu.VMEM((2 * NZ, SEQ, 2 * WIDTH), BF),
            pltpu.VMEM((NZ, SEQ, 2 * WIDTH), BF),
            pltpu.VMEM((NZ, SEQ, D), BF),
            pltpu.VMEM((6, HALF, D), BF),
            pltpu.VMEM((GROWS, D), BF),
            pltpu.VMEM((3, GROWS, D), BF),
            pltpu.VMEM((GROWS, D), BF),
            pltpu.VMEM((GROWS, D), BF),
            pltpu.VMEM((GROWS, D), BF),
            pltpu.VMEM((3, GROWS, D), BF),
            pltpu.VMEM((SEQ, D), BF),
            dma((6, 2, 2)), dma((6, 2, 2)),
            dma((4, 2)), dma((4, 2)),
            dma((4,)), dma((4,)),
            dma((6, 2)), dma((6, 2)),
            dma((3,)), dma((3,)),
            dma((9,)), dma((9,)),
            dma((7,)), dma((7,)),
            dma((6,)), dma((8,)),
        ],
        compiler_params=pltpu.CompilerParams(
            collective_id=0, has_side_effects=True, vmem_limit_bytes=67043328
        ),
    )(
        tokens[0], ln_gain[None], ln_bias[None],
        jnp.transpose(w_qkv, (1, 0, 2)), w_out, grad_partial[0],
    )
    mixed, grad_sum = pl.pallas_call(
        finish,
        out_shape=(
            jax.ShapeDtypeStruct((SEQ, D), BF),
            jax.ShapeDtypeStruct((WIDTH, D), F32),
        ),
        in_specs=[any_spec, any_spec],
        out_specs=(any_spec, any_spec),
        scratch_shapes=[
            pltpu.VMEM((SEQ, D), BF),
            pltpu.VMEM((WIDTH, D), BF),
            pltpu.VMEM((WIDTH, D), F32),
            dma((NG + NM,)), dma((NG + NM,)),
        ],
    )(mixed, grad_sum)
    return (mixed[None], grad_sum)


def solution(mesh):
    placed = (
        P("dp", "mp", None),
        P(),
        P(),
        P(None, None, "mp"),
        P("mp", None),
        P("dp", "mp", None),
    )
    return jax.shard_map(
        body,
        mesh=mesh,
        in_specs=placed,
        out_specs=(P("dp", "mp", None), P("mp", None)),
        check_vma=False,
    )
```

```python
import jax
import jax.numpy as jnp
from jax import lax
from jax.experimental import pallas as pl
from jax.experimental.pallas import tpu as pltpu
from jax.sharding import PartitionSpec as P

HEAD = 128
SEQ = 128
D = 5120
NY = 4
NZ = 4
WIDTH = 256
HALF = SEQ // 2
QUART = SEQ // 4
GROWS = WIDTH // NY
MESH = pl.DeviceIdType.MESH
BF = jnp.bfloat16
F32 = jnp.float32


def attend(query, keys, values):
    scores = lax.dot_general(
        query, keys, (((1,), (1,)), ((), ())), preferred_element_type=F32
    ) * HEAD ** (-0.5)
    scaled = scores - jnp.max(scores, axis=-1, keepdims=True)
    expsc = jnp.exp(scaled)
    attn = (expsc / jnp.sum(expsc, axis=-1, keepdims=True)).astype(BF)
    return jnp.dot(attn, values, preferred_element_type=F32).astype(BF)


def kernel(
    tok_hbm, gain, bias, wq_hbm, wo_hbm, g_hbm,
    mixed_hbm, gsum_hbm,
    raw, T, WQ, WO, QKV, CTX, CTXR, PS, RB,
    GO, GR, GX, GXR, GT, GA, OM,
    zs, zr, xs, xr, cs, cr, rss, rsr,
    wqs, wqr, wos, wor, gs, gr, loc, outs,
):
    dp = lax.axis_index("dp")
    mp = lax.axis_index("mp")
    y, xl = dp // 2, dp % 2
    xh, z, c = mp // 8, (mp // 2) % 4, mp % 2

    def dev(y, xl, xh, z, c):
        return (lax.rem(y + NY, NY) * 2 + xl, xh * 8 + lax.rem(z + NZ, NZ) * 2 + c)

    zdev = (dev(y, xl, xh, z + 1, c), dev(y, xl, xh, z - 1, c))
    x2 = dev(y, xl, 1 - xh, z, c)
    mate = dev(y, xl, xh, z, 1 - c)
    cross = dev(y, 1 - xl, 1 - xh, z, c)
    xlo = dev(y, 1 - xl, xh, z, c)
    ydev = [dev(y + k, xl, xh, z, c) for k in (1, 2, 3 - NY)]

    def local(src, dst, sem):
        copy = pltpu.make_async_copy(src, dst, sem)
        copy.start()
        return copy

    def quarter(h, q):
        return pl.ds(h * HALF + q * QUART, QUART)

    load_raw = [
        [local(tok_hbm.at[quarter(h, q)], raw.at[quarter(h, q)], loc.at[6 + 2 * q + h]) for h in range(2)]
        for q in range(2)
    ]
    load_wq = [local(wq_hbm.at[j], WQ.at[c * 3 + j], loc.at[1 + j]) for j in range(3)]
    own_seg = pl.multiple_of((xh * 2 + c) * WIDTH, WIDTH)
    far_seg = pl.multiple_of(((1 - xh) * 2 + c) * WIDTH, WIDTH)
    load_wo = local(wo_hbm, WO.at[pl.ds(own_seg, WIDTH)], loc.at[4])
    my_rows = pl.ds(pl.multiple_of(y * GROWS, GROWS), GROWS)
    load_g = local(g_hbm.at[my_rows], GO, loc.at[5])

    barrier = pltpu.get_barrier_semaphore()
    peers = [*zdev, x2, mate, cross, xlo, *ydev]
    for peer in peers:
        pl.semaphore_signal(barrier, inc=1, device_id=peer, device_id_type=MESH)

    def slot(col, zz):
        return col * NZ + lax.rem(zz + 2 * NZ, NZ)

    own = slot(xh, z)
    pl.semaphore_wait(barrier, len(peers))

    sent = []

    def send(src, dst, ssem, rsem, peer):
        copy = pltpu.make_async_remote_copy(
            src_ref=src, dst_ref=dst, send_sem=ssem, recv_sem=rsem,
            device_id=peer, device_id_type=MESH,
        )
        copy.start()
        sent.append(copy)
        return copy

    def part(seg, yy):
        return pl.ds(pl.multiple_of(seg + yy * GROWS, GROWS), GROWS)

    wo_cross = send(
        wo_hbm.at[part(0, y)], WO.at[part(own_seg, y)], wos.at[0], wor.at[0], cross
    )

    wq_mate = [
        send(wq_hbm.at[j], WQ.at[c * 3 + j], wqs.at[j], wqr.at[j], mate) for j in range(3)
    ]
    wo_mate = send(wo_hbm, WO.at[pl.ds(own_seg, WIDTH)], wos.at[1], wor.at[1], mate)
    g_rs = []
    for k in range(3):
        rows = pl.ds(pl.multiple_of(lax.rem(y + k + 1, NY) * GROWS, GROWS), GROWS)
        g_rs.append(send(g_hbm.at[rows], GR.at[k], gs.at[k], gr.at[k], ydev[k]))

    def project(s, base, count):
        @pl.loop(0, count)
        def _(j):
            QKV[base + j] = jnp.dot(T[s], WQ[base + j], preferred_element_type=F32).astype(BF)

    def attention(s):
        for cc in range(2):
            for h in range(2):
                cols = slice(h * HEAD, (h + 1) * HEAD)
                CTX[s, :, cc * WIDTH + h * HEAD:cc * WIDTH + (h + 1) * HEAD] = attend(
                    QKV[cc * 3, :, cols], QKV[cc * 3 + 1, :, cols], QKV[cc * 3 + 2, :, cols]
                )

    ccopy = {}

    def ctx_send(k):
        zz = lax.rem(z + k, NZ)
        ccopy[k] = send(CTX.at[slot(1 - xh, z + k)], CTXR.at[zz], cs.at[k], cr.at[k], x2)

    zcopy, xcopy = {}, {}

    def zsend(step, h, q, s):
        ref = T.at[s, quarter(h, q)]
        zcopy[step, h, q] = send(ref, ref, zs.at[step, h, q], zr.at[step, h, q], zdev[h])

    def xsend(step, h, q, s):
        ref = T.at[s, quarter(h, q)]
        xcopy[step, h] = send(ref, ref, xs.at[step, h], xr.at[step, h], x2)

    sign = (1, -1)
    for q in range(2):
        for h in range(2):
            load_raw[q][h].wait()

            @pl.loop(0, QUART // 16)
            def _(i, h=h, q=q):
                rows = pl.ds(pl.multiple_of(h * HALF + q * QUART + i * 16, 16), 16)
                values = raw[rows, :].astype(F32)
                center = jnp.mean(values, axis=-1, keepdims=True)
                spread = jnp.mean((values - center) * (values - center), axis=-1, keepdims=True)
                T[own, rows, :] = (
                    (values - center) * lax.rsqrt(spread + 1e-06) * gain[...] + bias[...]
                ).astype(BF)
            zsend(0, h, q, own)

    def by_rows(count, fn):
        @pl.loop(0, count // 16)
        def _(i):
            fn(pl.ds(pl.multiple_of(i * 16, 16), 16))

    for copy in load_wq:
        copy.wait()
    project(own, c * 3, 3)
    for h in range(2):
        zcopy[0, h, 0].wait_recv()
        zsend(1, h, 0, slot(xh, z - sign[h]))
    for copy in wq_mate:
        copy.wait_recv()
    project(own, (1 - c) * 3, 3)
    attention(own)

    wo_cross.wait_recv()
    for h in range(2):
        xsend(0, h, 1, own)
    rows = WO.at[part(far_seg, y)]
    wo_y = [send(rows, rows, wos.at[2 + k], wor.at[2 + k], ydev[k]) for k in range(3)]
    wo_fwd = [send(rows, rows, wos.at[5], wor.at[5], mate)]

    for h in range(2):
        zcopy[0, h, 1].wait_recv()
        zsend(1, h, 1, slot(xh, z - sign[h]))
    for h in range(2):
        zcopy[1, h, 0].wait_recv()
        zsend(2, h, 0, slot(xh, z + 2))
        xsend(1, h, 0, slot(xh, z + 2))
    for h in range(2):
        zcopy[1, h, 1].wait_recv()
        xcopy[0, h].wait_recv()
        zsend(3, h, 1, slot(1 - xh, z))
        zsend(2, h, 1, slot(xh, z + 2))
    project(slot(xh, z + 2), 0, 6)
    attention(slot(xh, z + 2))

    load_g.wait()
    for copy in g_rs:
        copy.wait_recv()

    def sum4(rows):
        GX[rows, :] = (
            (GO[rows, :].astype(F32) + GR[0, rows, :].astype(F32))
            + (GR[1, rows, :].astype(F32) + GR[2, rows, :].astype(F32))
        ).astype(BF)
    by_rows(GROWS, sum4)
    g_half = [pl.ds(i * (GROWS // 2), GROWS // 2) for i in range(2)]

    def g_swap(i):
        return send(GX.at[g_half[i]], GXR.at[g_half[i]], gs.at[3 + i], gr.at[3 + i], xlo)

    g_x = [g_swap(0)]
    for h in range(2):
        xsend(2, h, 0, slot(xh, z - sign[h]))

    for h in range(2):
        zcopy[3, h, 1].wait_recv()
        zsend(4, h, 1, slot(1 - xh, z - sign[h]))
    for h in range(2):
        xcopy[1, h].wait_recv()
        zsend(3, h, 0, slot(1 - xh, z + 2))
    for q in range(2):
        for h in range(2):
            zcopy[2, h, q].wait_recv()
    project(slot(xh, z + 1), 0, 6)
    attention(slot(xh, z + 1))

    for h in range(2):
        zcopy[4, h, 1].wait_recv()
        zsend(5, h, 1, slot(1 - xh, z + 2))
    project(slot(1 - xh, z + 2), 0, 6)
    attention(slot(1 - xh, z + 2))
    ctx_send(2)
    g_x.append(g_swap(1))

    for k in range(3):
        wo_y[k].wait_recv()
        rows = WO.at[part(far_seg, lax.rem(y + NY - k - 1, NY))]
        wo_fwd.append(send(rows, rows, wos.at[6 + k], wor.at[6 + k], mate))
    project(slot(xh, z + 3), 0, 6)
    attention(slot(xh, z + 3))

    load_wo.wait()
    wo_mate.wait_recv()
    for copy in wo_fwd:
        copy.wait_recv()

    def out_project(k):
        zz = lax.rem(z + k, NZ)
        near = pl.ds(pl.multiple_of(xh * 2 * WIDTH, WIDTH), 2 * WIDTH)
        far = pl.ds(pl.multiple_of((1 - xh) * 2 * WIDTH, WIDTH), 2 * WIDTH)

        @pl.loop(0, D // 512)
        def _(j):
            cols = pl.ds(pl.multiple_of(j * 512, 512), 512)
            PS[zz, :, cols] = (
                jnp.dot(CTX[slot(xh, zz)], WO[near, cols], preferred_element_type=F32)
                + jnp.dot(CTXR[zz], WO[far, cols], preferred_element_type=F32)
            ).astype(BF)

    ccopy[2].wait_recv()
    out_project(2)

    rcopy = {}

    def rsend(kind, q, image, h, to):
        ref = PS.at[lax.rem(image + 2 * NZ, NZ), quarter(h, q)]
        rcopy[kind, q] = send(
            ref, RB.at[kind, pl.ds(q * QUART, QUART)],
            rss.at[kind, q], rsr.at[kind, q], zdev[to],
        )

    for q in range(2):
        rsend(0, q, z + 2, 0, 1)
        rsend(1, q, z + 2, 1, 0)

    for h in range(2):
        zcopy[3, h, 0].wait_recv()
        zcopy[5, h, 1].wait_recv()
        xcopy[2, h].wait_recv()
    for k in (1, 3):
        project(slot(1 - xh, z + k), 0, 6)
        attention(slot(1 - xh, z + k))
        ctx_send(k)
    for h in range(2):
        xsend(3, h, 0, own)

    for copy in g_x:
        copy.wait_recv()

    def sum2(rows):
        GT[rows, :] = (GX[rows, :].astype(F32) + GXR[rows, :].astype(F32)).astype(BF)
    by_rows(GROWS, sum2)
    g_ag = [send(GT, GA.at[k], gs.at[5 + k], gr.at[5 + k], ydev[k]) for k in range(3)]

    ccopy[1].wait_recv()
    out_project(1)
    for q in range(2):
        rsend(4, q, z + 1, 0, 0)
    ccopy[3].wait_recv()
    out_project(3)
    for q in range(2):
        rsend(5, q, z - 1, 1, 1)

    for q in range(2):
        for h in range(2):
            image = lax.rem(z - sign[h] + NZ, NZ)
            rcopy[h, q].wait_recv()

            @pl.loop(0, QUART // 16)
            def _(i, h=h, q=q, image=image):
                at = pl.multiple_of(q * QUART + i * 16, 16)
                rows = pl.ds(h * HALF + at, 16)
                PS[image, rows, :] = (
                    PS[image, rows, :].astype(F32) + RB[h, pl.ds(at, 16), :].astype(F32)
                ).astype(BF)
            rsend(2 + h, q, z - sign[h], h, 1 - h)

    for h in range(2):
        xcopy[3, h].wait_recv()
    project(slot(1 - xh, z), 0, 6)
    attention(slot(1 - xh, z))
    ctx_send(0)
    ccopy[0].wait_recv()
    out_project(0)

    for copy in sent[:-9]:
        copy.wait_send()

    written = [local(GT, gsum_hbm.at[my_rows], outs.at[0])]
    for k in range(3):
        g_ag[k].wait_recv()
        rows = pl.ds(pl.multiple_of(lax.rem(y + NY - k - 1, NY) * GROWS, GROWS), GROWS)
        written.append(local(GA.at[k], gsum_hbm.at[rows], outs.at[1 + k]))

    for q in range(2):
        for h in range(2):
            rcopy[4 + h, q].wait_recv()
            rcopy[2 + h, q].wait_recv()

            @pl.loop(0, QUART // 16)
            def _(i, h=h, q=q):
                at = pl.multiple_of(q * QUART + i * 16, 16)
                rows = pl.ds(h * HALF + at, 16)
                part = pl.ds(at, 16)
                proj = PS[z, rows, :].astype(F32) + (
                    RB[2 + h, part, :].astype(F32) + RB[4 + h, part, :].astype(F32)
                )
                OM[rows, :] = (raw[rows, :].astype(F32) + proj).astype(BF)
            written.append(
                local(OM.at[quarter(h, q)], mixed_hbm.at[quarter(h, q)], outs.at[4 + h * 2 + q])
            )
    for copy in written:
        copy.wait()
    for copy in sent[-9:]:
        copy.wait_send()


NG = 8
NM = 2


def finish(mixed_in, grad_in, mixed_out, grad_out, held, narrow, wide, isem, osem):
    def chunk(n, i, total):
        return pl.ds(i * (total // n), total // n)

    def copy(src, dst, sem):
        made = pltpu.make_async_copy(src, dst, sem)
        made.start()
        return made

    grads = [chunk(NG, i, WIDTH) for i in range(NG)]
    rows = [chunk(NM, i, SEQ) for i in range(NM)]
    came = [copy(grad_in.at[r], narrow.at[r], isem.at[i]) for i, r in enumerate(grads)]
    came += [copy(mixed_in.at[r], held.at[r], isem.at[NG + i]) for i, r in enumerate(rows)]
    left = []
    for i, r in enumerate(grads):
        came[i].wait()

        @pl.loop(0, WIDTH // NG // 16)
        def _(j, i=i):
            at = pl.ds(pl.multiple_of(i * (WIDTH // NG) + j * 16, 16), 16)
            wide[at, :] = narrow[at, :].astype(F32)
        left.append(copy(wide.at[r], grad_out.at[r], osem.at[i]))
    for i, r in enumerate(rows):
        came[NG + i].wait()
        left.append(copy(held.at[r], mixed_out.at[r], osem.at[NG + i]))
    for made in left:
        made.wait()


def body(tokens, ln_gain, ln_bias, w_qkv, w_out, grad_partial):
    dma = pltpu.SemaphoreType.DMA
    any_spec = pl.BlockSpec(memory_space=pl.ANY)
    vmem = pl.BlockSpec(memory_space=pltpu.VMEM)
    mixed, grad_sum = pl.pallas_call(
        kernel,
        out_shape=(
            jax.ShapeDtypeStruct((SEQ, D), BF),
            jax.ShapeDtypeStruct((WIDTH, D), BF),
        ),
        in_specs=[any_spec, vmem, vmem, any_spec, any_spec, any_spec],
        out_specs=(any_spec, any_spec),
        scratch_shapes=[
            pltpu.VMEM((SEQ, D), BF),
            pltpu.VMEM((2 * NZ, SEQ, D), BF),
            pltpu.VMEM((6, D, WIDTH), BF),
            pltpu.VMEM((4 * WIDTH, D), BF),
            pltpu.VMEM((6, SEQ, WIDTH), BF),
            pltpu.VMEM((2 * NZ, SEQ, 2 * WIDTH), BF),
            pltpu.VMEM((NZ, SEQ, 2 * WIDTH), BF),
            pltpu.VMEM((NZ, SEQ, D), BF),
            pltpu.VMEM((6, HALF, D), BF),
            pltpu.VMEM((GROWS, D), BF),
            pltpu.VMEM((3, GROWS, D), BF),
            pltpu.VMEM((GROWS, D), BF),
            pltpu.VMEM((GROWS, D), BF),
            pltpu.VMEM((GROWS, D), BF),
            pltpu.VMEM((3, GROWS, D), BF),
            pltpu.VMEM((SEQ, D), BF),
            dma((6, 2, 2)), dma((6, 2, 2)),
            dma((4, 2)), dma((4, 2)),
            dma((4,)), dma((4,)),
            dma((6, 2)), dma((6, 2)),
            dma((3,)), dma((3,)),
            dma((9,)), dma((9,)),
            dma((8,)), dma((8,)),
            dma((10,)), dma((8,)),
        ],
        compiler_params=pltpu.CompilerParams(
            collective_id=0, has_side_effects=True, vmem_limit_bytes=67043328
        ),
    )(
        tokens[0], ln_gain[None], ln_bias[None],
        jnp.transpose(w_qkv, (1, 0, 2)), w_out, grad_partial[0],
    )
    mixed, grad_sum = pl.pallas_call(
        finish,
        out_shape=(
            jax.ShapeDtypeStruct((SEQ, D), BF),
            jax.ShapeDtypeStruct((WIDTH, D), F32),
        ),
        in_specs=[any_spec, any_spec],
        out_specs=(any_spec, any_spec),
        scratch_shapes=[
            pltpu.VMEM((SEQ, D), BF),
            pltpu.VMEM((WIDTH, D), BF),
            pltpu.VMEM((WIDTH, D), F32),
            dma((NG + NM,)), dma((NG + NM,)),
        ],
    )(mixed, grad_sum)
    return (mixed[None], grad_sum)


def solution(mesh):
    placed = (
        P("dp", "mp", None),
        P(),
        P(),
        P(None, None, "mp"),
        P("mp", None),
        P("dp", "mp", None),
    )
    return jax.shard_map(
        body,
        mesh=mesh,
        in_specs=placed,
        out_specs=(P("dp", "mp", None), P("mp", None)),
        check_vma=False,
    )
```

```python
import jax
import jax.numpy as jnp
from jax import lax
from jax.experimental import pallas as pl
from jax.experimental.pallas import tpu as pltpu
from jax.sharding import PartitionSpec as P

HEAD = 128
SEQ = 128
D = 5120
NY = 4
NZ = 4
WIDTH = 256
HALF = SEQ // 2
QUART = SEQ // 4
GROWS = WIDTH // NY
MESH = pl.DeviceIdType.MESH
BF = jnp.bfloat16
F32 = jnp.float32


def attend(query, keys, values):
    scores = lax.dot_general(
        query, keys, (((1,), (1,)), ((), ())), preferred_element_type=F32
    ) * HEAD ** (-0.5)
    scaled = scores - jnp.max(scores, axis=-1, keepdims=True)
    expsc = jnp.exp(scaled)
    attn = (expsc / jnp.sum(expsc, axis=-1, keepdims=True)).astype(BF)
    return jnp.dot(attn, values, preferred_element_type=F32).astype(BF)


def kernel(
    tok_hbm, gain, bias, wq_hbm, wo_hbm, g_hbm,
    OM, gsum,
    raw, T, WQ, WO, QKV, CTX, CTXR, PS, RB,
    GO, GR, GX, GXR, GT, GA,
    zs, zr, xs, xr, cs, cr, rss, rsr,
    wqs, wqr, wos, wor, gs, gr, loc,
):
    dp = lax.axis_index("dp")
    mp = lax.axis_index("mp")
    y, xl = dp // 2, dp % 2
    xh, z, c = mp // 8, (mp // 2) % 4, mp % 2

    def dev(y, xl, xh, z, c):
        return (lax.rem(y + NY, NY) * 2 + xl, xh * 8 + lax.rem(z + NZ, NZ) * 2 + c)

    zdev = (dev(y, xl, xh, z + 1, c), dev(y, xl, xh, z - 1, c))
    x2 = dev(y, xl, 1 - xh, z, c)
    mate = dev(y, xl, xh, z, 1 - c)
    cross = dev(y, 1 - xl, 1 - xh, z, c)
    xlo = dev(y, 1 - xl, xh, z, c)
    ydev = [dev(y + k, xl, xh, z, c) for k in (1, 2, 3 - NY)]

    barrier = pltpu.get_barrier_semaphore()
    peers = [*zdev, x2, mate, cross, xlo, *ydev]
    for peer in peers:
        pl.semaphore_signal(barrier, inc=1, device_id=peer, device_id_type=MESH)

    def local(src, dst, sem):
        copy = pltpu.make_async_copy(src, dst, sem)
        copy.start()
        return copy

    def quarter(h, q):
        return pl.ds(h * HALF + q * QUART, QUART)

    load_raw = [
        [local(tok_hbm.at[quarter(h, q)], raw.at[quarter(h, q)], loc.at[6 + 2 * q + h]) for h in range(2)]
        for q in range(2)
    ]
    load_wq = [local(wq_hbm.at[j], WQ.at[c * 3 + j], loc.at[1 + j]) for j in range(3)]
    own_seg = pl.multiple_of((xh * 2 + c) * WIDTH, WIDTH)
    far_seg = pl.multiple_of(((1 - xh) * 2 + c) * WIDTH, WIDTH)
    load_wo = local(wo_hbm, WO.at[pl.ds(own_seg, WIDTH)], loc.at[4])
    my_rows = pl.ds(pl.multiple_of(y * GROWS, GROWS), GROWS)
    load_g = local(g_hbm.at[my_rows], GO, loc.at[5])

    def slot(col, zz):
        return col * NZ + lax.rem(zz + 2 * NZ, NZ)

    own = slot(xh, z)
    def norm_rows(h, q):
        load_raw[q][h].wait()

        @pl.loop(0, QUART // 16)
        def _(i):
            rows = pl.ds(pl.multiple_of(h * HALF + q * QUART + i * 16, 16), 16)
            values = raw[rows, :].astype(F32)
            center = jnp.mean(values, axis=-1, keepdims=True)
            spread = jnp.mean((values - center) * (values - center), axis=-1, keepdims=True)
            T[own, rows, :] = (
                (values - center) * lax.rsqrt(spread + 1e-06) * gain[...] + bias[...]
            ).astype(BF)

    for h in range(2):
        norm_rows(h, 0)
    pl.semaphore_wait(barrier, len(peers))

    sent = []

    def send(src, dst, ssem, rsem, peer):
        copy = pltpu.make_async_remote_copy(
            src_ref=src, dst_ref=dst, send_sem=ssem, recv_sem=rsem,
            device_id=peer, device_id_type=MESH,
        )
        copy.start()
        sent.append(copy)
        return copy

    def part(seg, yy):
        return pl.ds(pl.multiple_of(seg + yy * GROWS, GROWS), GROWS)

    wo_cross = send(
        wo_hbm.at[part(0, y)], WO.at[part(own_seg, y)], wos.at[0], wor.at[0], cross
    )

    zcopy, xcopy = {}, {}

    def zsend(step, h, q, s):
        ref = T.at[s, quarter(h, q)]
        zcopy[step, h, q] = send(ref, ref, zs.at[step, h, q], zr.at[step, h, q], zdev[h])

    def xsend(step, h, q, s):
        ref = T.at[s, quarter(h, q)]
        xcopy[step, h] = send(ref, ref, xs.at[step, h], xr.at[step, h], x2)

    sign = (1, -1)
    for h in range(2):
        zsend(0, h, 0, own)
    wq_mate = [
        send(wq_hbm.at[j], WQ.at[c * 3 + j], wqs.at[j], wqr.at[j], mate) for j in range(3)
    ]
    wo_mate = send(wo_hbm, WO.at[pl.ds(own_seg, WIDTH)], wos.at[1], wor.at[1], mate)
    g_rs = []
    for k in range(3):
        rows = pl.ds(pl.multiple_of(lax.rem(y + k + 1, NY) * GROWS, GROWS), GROWS)
        g_rs.append(send(g_hbm.at[rows], GR.at[k], gs.at[k], gr.at[k], ydev[k]))

    def project(s, base, count):
        @pl.loop(0, count)
        def _(j):
            QKV[0, base + j] = jnp.dot(T[s], WQ[base + j], preferred_element_type=F32).astype(BF)

    def project_pair(col, way):
        up, down = slot(col, z + 1), slot(col, z + 3)
        at_up, at_down = (1 - way) * HALF, way * HALF

        @pl.loop(0, 6)
        def _(j):
            lhs = jnp.concatenate(
                [T[up, at_up:at_up + HALF], T[down, at_down:at_down + HALF]], axis=0
            )
            both = jnp.dot(lhs, WQ[j], preferred_element_type=F32).astype(BF)
            QKV[1, j, at_up:at_up + HALF] = both[:HALF]
            QKV[2, j, at_down:at_down + HALF] = both[HALF:]

    def attention(s, b=0):
        for cc in range(2):
            for h in range(2):
                cols = slice(h * HEAD, (h + 1) * HEAD)
                CTX[s, :, cc * WIDTH + h * HEAD:cc * WIDTH + (h + 1) * HEAD] = attend(
                    QKV[b, cc * 3, :, cols], QKV[b, cc * 3 + 1, :, cols],
                    QKV[b, cc * 3 + 2, :, cols],
                )

    ccopy = {}

    def ctx_send(k):
        zz = lax.rem(z + k, NZ)
        ccopy[k] = send(CTX.at[slot(1 - xh, z + k)], CTXR.at[zz], cs.at[k], cr.at[k], x2)
    for h in range(2):
        norm_rows(h, 1)
        zsend(0, h, 1, own)

    def by_rows(count, fn):
        @pl.loop(0, count // 16)
        def _(i):
            fn(pl.ds(pl.multiple_of(i * 16, 16), 16))

    for copy in load_wq:
        copy.wait()
    project(own, c * 3, 3)
    for h in range(2):
        zcopy[0, h, 0].wait_recv()
        zsend(1, h, 0, slot(xh, z - sign[h]))
    for copy in wq_mate:
        copy.wait_recv()
    project(own, (1 - c) * 3, 3)
    attention(own)

    wo_cross.wait_recv()
    for h in range(2):
        xsend(0, h, 1, own)
    rows = WO.at[part(far_seg, y)]
    wo_y = [send(rows, rows, wos.at[2 + k], wor.at[2 + k], ydev[k]) for k in range(3)]
    wo_fwd = [send(rows, rows, wos.at[5], wor.at[5], mate)]

    for h in range(2):
        zcopy[0, h, 1].wait_recv()
        zsend(1, h, 1, slot(xh, z - sign[h]))
    project_pair(xh, 0)
    for h in range(2):
        zcopy[1, h, 0].wait_recv()
        zsend(2, h, 0, slot(xh, z + 2))
        xsend(1, h, 0, slot(xh, z + 2))
    for h in range(2):
        zcopy[1, h, 1].wait_recv()
        xcopy[0, h].wait_recv()
        zsend(3, h, 1, slot(1 - xh, z))
        zsend(2, h, 1, slot(xh, z + 2))
    project(slot(xh, z + 2), 0, 6)
    attention(slot(xh, z + 2))

    load_g.wait()
    for copy in g_rs:
        copy.wait_recv()

    def sum4(rows):
        GX[rows, :] = (
            (GO[rows, :].astype(F32) + GR[0, rows, :].astype(F32))
            + (GR[1, rows, :].astype(F32) + GR[2, rows, :].astype(F32))
        ).astype(BF)
    by_rows(GROWS, sum4)
    g_half = [pl.ds(i * (GROWS // 2), GROWS // 2) for i in range(2)]

    def g_swap(i):
        return send(GX.at[g_half[i]], GXR.at[g_half[i]], gs.at[3 + i], gr.at[3 + i], xlo)

    g_x = [g_swap(0)]
    for h in range(2):
        xsend(2, h, 0, slot(xh, z - sign[h]))

    for h in range(2):
        zcopy[3, h, 1].wait_recv()
        zsend(4, h, 1, slot(1 - xh, z - sign[h]))
    for h in range(2):
        xcopy[1, h].wait_recv()
        zsend(3, h, 0, slot(1 - xh, z + 2))
    for q in range(2):
        for h in range(2):
            zcopy[2, h, q].wait_recv()
    project_pair(xh, 1)
    attention(slot(xh, z + 1), 1)
    attention(slot(xh, z + 3), 2)

    for h in range(2):
        zcopy[4, h, 1].wait_recv()
        zsend(5, h, 1, slot(1 - xh, z + 2))
    project(slot(1 - xh, z + 2), 0, 6)
    attention(slot(1 - xh, z + 2))
    ctx_send(2)
    g_x.append(g_swap(1))

    for k in range(3):
        wo_y[k].wait_recv()
        rows = WO.at[part(far_seg, lax.rem(y + NY - k - 1, NY))]
        wo_fwd.append(send(rows, rows, wos.at[6 + k], wor.at[6 + k], mate))
    for h in range(2):
        xcopy[2, h].wait_recv()
    project_pair(1 - xh, 0)

    load_wo.wait()
    wo_mate.wait_recv()
    for copy in wo_fwd:
        copy.wait_recv()

    def out_tiles(fn):
        @pl.loop(0, D // 512)
        def _(j):
            fn(pl.ds(pl.multiple_of(j * 512, 512), 512))

    near = pl.ds(pl.multiple_of(xh * 2 * WIDTH, WIDTH), 2 * WIDTH)
    far = pl.ds(pl.multiple_of((1 - xh) * 2 * WIDTH, WIDTH), 2 * WIDTH)

    def out_rows(pieces):
        def joined(ref_at):
            parts = [ref_at(k, start, count) for k, start, count in pieces]
            return parts[0] if len(parts) == 1 else jnp.concatenate(parts, axis=0)

        def tile(cols):
            mine = joined(lambda k, start, count: CTX[slot(xh, z + k), start:start + count])
            theirs = joined(lambda k, start, count: CTXR[lax.rem(z + k, NZ), start:start + count])
            made = (
                jnp.dot(mine, WO[near, cols], preferred_element_type=F32)
                + jnp.dot(theirs, WO[far, cols], preferred_element_type=F32)
            ).astype(BF)
            at = 0
            for k, start, count in pieces:
                PS[lax.rem(z + k, NZ), start:start + count, cols] = made[at:at + count]
                at += count
        out_tiles(tile)

    ccopy[2].wait_recv()
    out_rows([(2, 0, SEQ)])

    rcopy = {}

    def rsend(kind, q, image, h, to):
        ref = PS.at[lax.rem(image + 2 * NZ, NZ), quarter(h, q)]
        rcopy[kind, q] = send(
            ref, RB.at[kind, pl.ds(q * QUART, QUART)],
            rss.at[kind, q], rsr.at[kind, q], zdev[to],
        )

    for q in range(2):
        rsend(0, q, z + 2, 0, 1)
        rsend(1, q, z + 2, 1, 0)

    for h in range(2):
        zcopy[3, h, 0].wait_recv()
        zcopy[5, h, 1].wait_recv()
    project_pair(1 - xh, 1)
    for k in (1, 3):
        attention(slot(1 - xh, z + k), (k + 1) // 2)
        ctx_send(k)
    for h in range(2):
        xsend(3, h, 0, own)

    for copy in g_x:
        copy.wait_recv()

    def sum2(rows):
        GT[rows, :] = (GX[rows, :].astype(F32) + GXR[rows, :].astype(F32)).astype(BF)
    by_rows(GROWS, sum2)
    g_ag = [send(GT, GA.at[k], gs.at[5 + k], gr.at[5 + k], ydev[k]) for k in range(3)]

    ccopy[1].wait_recv()
    ccopy[3].wait_recv()
    out_rows([(1, 0, HALF), (3, HALF, HALF)])
    for q in range(2):
        rsend(4, q, z + 1, 0, 0)
        rsend(5, q, z - 1, 1, 1)
    out_rows([(1, HALF, HALF), (3, 0, HALF)])

    for q in range(2):
        for h in range(2):
            image = lax.rem(z - sign[h] + NZ, NZ)
            rcopy[h, q].wait_recv()

            @pl.loop(0, QUART // 16)
            def _(i, h=h, q=q, image=image):
                at = pl.multiple_of(q * QUART + i * 16, 16)
                rows = pl.ds(h * HALF + at, 16)
                PS[image, rows, :] = (
                    PS[image, rows, :].astype(F32) + RB[h, pl.ds(at, 16), :].astype(F32)
                ).astype(BF)
            rsend(2 + h, q, z - sign[h], h, 1 - h)

    for h in range(2):
        xcopy[3, h].wait_recv()
    project(slot(1 - xh, z), 0, 6)
    attention(slot(1 - xh, z))
    ctx_send(0)
    ccopy[0].wait_recv()
    out_rows([(0, 0, SEQ)])

    for copy in sent[:-9]:
        copy.wait_send()

    for k in range(4):
        if k:
            g_ag[k - 1].wait_recv()
        base = lax.rem(y + NY - k, NY) * GROWS

        def place(rows, k=k, base=base):
            part = GT[rows, :] if k == 0 else GA[k - 1, rows, :]
            gsum[pl.ds(pl.multiple_of(base + rows.start, 16), 16), :] = part.astype(F32)
        by_rows(GROWS, place)

    for q in range(2):
        for h in range(2):
            rcopy[4 + h, q].wait_recv()
            rcopy[2 + h, q].wait_recv()

            @pl.loop(0, QUART // 16)
            def _(i, h=h, q=q):
                at = pl.multiple_of(q * QUART + i * 16, 16)
                rows = pl.ds(h * HALF + at, 16)
                part = pl.ds(at, 16)
                proj = PS[z, rows, :].astype(F32) + (
                    RB[2 + h, part, :].astype(F32) + RB[4 + h, part, :].astype(F32)
                )
                OM[rows, :] = (raw[rows, :].astype(F32) + proj).astype(BF)
    for copy in sent[-9:]:
        copy.wait_send()


def finish(mixed_in, grad_in, mixed_out, grad_out, sem):
    made = [pltpu.make_async_copy(mixed_in, mixed_out, sem.at[4])]
    for i in range(4):
        rows = pl.ds(i * GROWS, GROWS)
        made.append(pltpu.make_async_copy(grad_in.at[rows], grad_out.at[rows], sem.at[i]))
    for copy in made:
        copy.start()
    for copy in made:
        copy.wait()


def body(tokens, ln_gain, ln_bias, w_qkv, w_out, grad_partial):
    dma = pltpu.SemaphoreType.DMA
    any_spec = pl.BlockSpec(memory_space=pl.ANY)
    vmem = pl.BlockSpec(memory_space=pltpu.VMEM)
    mixed, grad_sum = pl.pallas_call(
        kernel,
        out_shape=(pltpu.VMEM((SEQ, D), BF), pltpu.VMEM((WIDTH, D), F32)),
        in_specs=[any_spec, vmem, vmem, any_spec, any_spec, any_spec],
        out_specs=(vmem, vmem),
        scratch_shapes=[
            pltpu.VMEM((SEQ, D), BF),
            pltpu.VMEM((2 * NZ, SEQ, D), BF),
            pltpu.VMEM((6, D, WIDTH), BF),
            pltpu.VMEM((4 * WIDTH, D), BF),
            pltpu.VMEM((3, 6, SEQ, WIDTH), BF),
            pltpu.VMEM((2 * NZ, SEQ, 2 * WIDTH), BF),
            pltpu.VMEM((NZ, SEQ, 2 * WIDTH), BF),
            pltpu.VMEM((NZ, SEQ, D), BF),
            pltpu.VMEM((6, HALF, D), BF),
            pltpu.VMEM((GROWS, D), BF),
            pltpu.VMEM((3, GROWS, D), BF),
            pltpu.VMEM((GROWS, D), BF),
            pltpu.VMEM((GROWS, D), BF),
            pltpu.VMEM((GROWS, D), BF),
            pltpu.VMEM((3, GROWS, D), BF),
            dma((6, 2, 2)), dma((6, 2, 2)),
            dma((4, 2)), dma((4, 2)),
            dma((4,)), dma((4,)),
            dma((6, 2)), dma((6, 2)),
            dma((3,)), dma((3,)),
            dma((9,)), dma((9,)),
            dma((8,)), dma((8,)),
            dma((10,)),
        ],
        compiler_params=pltpu.CompilerParams(
            collective_id=0, has_side_effects=True, vmem_limit_bytes=57671680
        ),
    )(
        tokens[0], ln_gain[None], ln_bias[None],
        jnp.transpose(w_qkv, (1, 0, 2)), w_out, grad_partial[0],
    )
    mixed = pltpu.with_memory_space_constraint(mixed, pltpu.VMEM)
    grad_sum = pltpu.with_memory_space_constraint(grad_sum, pltpu.VMEM)
    mixed, grad_sum = pl.pallas_call(
        finish,
        out_shape=(
            jax.ShapeDtypeStruct((SEQ, D), BF),
            jax.ShapeDtypeStruct((WIDTH, D), F32),
        ),
        in_specs=[vmem, vmem],
        out_specs=(any_spec, any_spec),
        scratch_shapes=[dma((5,))],
        compiler_params=pltpu.CompilerParams(vmem_limit_bytes=1 << 20),
    )(mixed, grad_sum)
    return (mixed[None], grad_sum)


def solution(mesh):
    placed = (
        P("dp", "mp", None),
        P(),
        P(),
        P(None, None, "mp"),
        P("mp", None),
        P("dp", "mp", None),
    )
    return jax.shard_map(
        body,
        mesh=mesh,
        in_specs=placed,
        out_specs=(P("dp", "mp", None), P("mp", None)),
        check_vma=False,
    )
```

```python
import jax
import jax.numpy as jnp
from jax import lax
from jax.experimental import pallas as pl
from jax.experimental.pallas import tpu as pltpu
from jax.sharding import PartitionSpec as P

HEAD = 128
SEQ = 128
D = 5120
NY = 4
NZ = 4
WIDTH = 256
HALF = SEQ // 2
QUART = SEQ // 4
GROWS = WIDTH // NY
MESH = pl.DeviceIdType.MESH
BF = jnp.bfloat16
F32 = jnp.float32


def attend(heads):
    scores = [
        lax.dot_general(query, keys, (((1,), (1,)), ((), ())), preferred_element_type=F32)
        * HEAD ** (-0.5)
        for query, keys, _ in heads
    ]
    tops = [jnp.max(part, axis=-1, keepdims=True) for part in scores]
    expsc = [jnp.exp(part - top) for part, top in zip(scores, tops)]
    sums = [jnp.sum(part, axis=-1, keepdims=True) for part in expsc]
    attn = [(part / total).astype(BF) for part, total in zip(expsc, sums)]
    return [
        jnp.dot(part, values, preferred_element_type=F32).astype(BF)
        for part, (_, _, values) in zip(attn, heads)
    ]


def kernel(
    tok_hbm, gain, bias, wq_hbm, wo_hbm, g_hbm,
    OM, gsum,
    raw, T, WQ, WO, QKV, CTX, CTXR, PS, RB,
    GO, GR, GX, GXR, GT, GA,
    zs, zr, xs, xr, cs, cr, rss, rsr,
    wqs, wqr, wos, wor, gs, gr, loc,
):
    dp = lax.axis_index("dp")
    mp = lax.axis_index("mp")
    y, xl = dp // 2, dp % 2
    xh, z, c = mp // 8, (mp // 2) % 4, mp % 2

    def dev(y, xl, xh, z, c):
        return (lax.rem(y + NY, NY) * 2 + xl, xh * 8 + lax.rem(z + NZ, NZ) * 2 + c)

    zdev = (dev(y, xl, xh, z + 1, c), dev(y, xl, xh, z - 1, c))
    x2 = dev(y, xl, 1 - xh, z, c)
    mate = dev(y, xl, xh, z, 1 - c)
    cross = dev(y, 1 - xl, 1 - xh, z, c)
    xlo = dev(y, 1 - xl, xh, z, c)
    ydev = [dev(y + k, xl, xh, z, c) for k in (1, 2, 3 - NY)]

    barrier = pltpu.get_barrier_semaphore()
    peers = [*zdev, x2, mate, cross, xlo, *ydev]
    for peer in peers:
        pl.semaphore_signal(barrier, inc=1, device_id=peer, device_id_type=MESH)

    def local(src, dst, sem):
        copy = pltpu.make_async_copy(src, dst, sem)
        copy.start()
        return copy

    def quarter(h, q):
        return pl.ds(h * HALF + q * QUART, QUART)

    load_raw = [
        [local(tok_hbm.at[quarter(h, q)], raw.at[quarter(h, q)], loc.at[6 + 2 * q + h]) for h in range(2)]
        for q in range(2)
    ]
    load_wq = [local(wq_hbm.at[j], WQ.at[c * 3 + j], loc.at[1 + j]) for j in range(3)]
    own_seg = pl.multiple_of((xh * 2 + c) * WIDTH, WIDTH)
    far_seg = pl.multiple_of(((1 - xh) * 2 + c) * WIDTH, WIDTH)
    load_wo = local(wo_hbm, WO.at[pl.ds(own_seg, WIDTH)], loc.at[4])
    my_rows = pl.ds(pl.multiple_of(y * GROWS, GROWS), GROWS)
    load_g = local(g_hbm.at[my_rows], GO, loc.at[5])

    def slot(col, zz):
        return col * NZ + lax.rem(zz + 2 * NZ, NZ)

    own = slot(xh, z)
    def norm_rows(h, q):
        load_raw[q][h].wait()

        @pl.loop(0, QUART // 16)
        def _(i):
            rows = pl.ds(pl.multiple_of(h * HALF + q * QUART + i * 16, 16), 16)
            values = raw[rows, :].astype(F32)
            center = jnp.mean(values, axis=-1, keepdims=True)
            spread = jnp.mean((values - center) * (values - center), axis=-1, keepdims=True)
            T[own, rows, :] = (
                (values - center) * lax.rsqrt(spread + 1e-06) * gain[...] + bias[...]
            ).astype(BF)

    for h in range(2):
        norm_rows(h, 0)
    pl.semaphore_wait(barrier, len(peers))

    sent = []

    def send(src, dst, ssem, rsem, peer):
        copy = pltpu.make_async_remote_copy(
            src_ref=src, dst_ref=dst, send_sem=ssem, recv_sem=rsem,
            device_id=peer, device_id_type=MESH,
        )
        copy.start()
        sent.append(copy)
        return copy

    def part(seg, yy):
        return pl.ds(pl.multiple_of(seg + yy * GROWS, GROWS), GROWS)

    wo_cross = send(
        wo_hbm.at[part(0, y)], WO.at[part(own_seg, y)], wos.at[0], wor.at[0], cross
    )

    zcopy, xcopy = {}, {}

    def zsend(step, h, q, s):
        ref = T.at[s, quarter(h, q)]
        zcopy[step, h, q] = send(ref, ref, zs.at[step, h, q], zr.at[step, h, q], zdev[h])

    def xsend(step, h, q, s):
        ref = T.at[s, quarter(h, q)]
        xcopy[step, h] = send(ref, ref, xs.at[step, h], xr.at[step, h], x2)

    sign = (1, -1)
    for h in range(2):
        zsend(0, h, 0, own)
    wq_mate = [
        send(wq_hbm.at[j], WQ.at[c * 3 + j], wqs.at[j], wqr.at[j], mate) for j in range(3)
    ]
    wo_mate = send(wo_hbm, WO.at[pl.ds(own_seg, WIDTH)], wos.at[1], wor.at[1], mate)
    g_rs = []
    for k in range(3):
        rows = pl.ds(pl.multiple_of(lax.rem(y + k + 1, NY) * GROWS, GROWS), GROWS)
        g_rs.append(send(g_hbm.at[rows], GR.at[k], gs.at[k], gr.at[k], ydev[k]))

    def project(s, base, count):
        @pl.loop(0, count)
        def _(j):
            QKV[0, base + j] = jnp.dot(T[s], WQ[base + j], preferred_element_type=F32).astype(BF)

    def project_pair(col, way):
        up, down = slot(col, z + 1), slot(col, z + 3)
        at_up, at_down = (1 - way) * HALF, way * HALF

        @pl.loop(0, 6)
        def _(j):
            lhs = jnp.concatenate(
                [T[up, at_up:at_up + HALF], T[down, at_down:at_down + HALF]], axis=0
            )
            both = jnp.dot(lhs, WQ[j], preferred_element_type=F32).astype(BF)
            QKV[1, j, at_up:at_up + HALF] = both[:HALF]
            QKV[2, j, at_down:at_down + HALF] = both[HALF:]

    def attention(*units):
        heads, places = [], []
        for s, b, start, count in units:
            rows = slice(start, start + count)
            for cc in range(2):
                for h in range(2):
                    cols = slice(h * HEAD, (h + 1) * HEAD)
                    heads.append((
                        QKV[b, cc * 3, rows, cols], QKV[b, cc * 3 + 1, :, cols],
                        QKV[b, cc * 3 + 2, :, cols],
                    ))
                    at = cc * WIDTH + h * HEAD
                    places.append((s, rows, slice(at, at + HEAD)))
        for place, made in zip(places, attend(heads)):
            CTX[place] = made

    def attend_all(s, b=0):
        attention((s, b, 0, SEQ))

    ccopy = {}

    def ctx_send(k, start=0, count=SEQ):
        rows = pl.ds(start, count)
        sems = (cs.at[k, start // HALF], cr.at[k, start // HALF])
        ccopy[k, start] = send(
            CTX.at[slot(1 - xh, z + k), rows], CTXR.at[lax.rem(z + k, NZ), rows], *sems, x2
        )

    for h in range(2):
        norm_rows(h, 1)
        zsend(0, h, 1, own)

    def by_rows(count, fn):
        @pl.loop(0, count // 16)
        def _(i):
            fn(pl.ds(pl.multiple_of(i * 16, 16), 16))

    for copy in load_wq:
        copy.wait()
    project(own, c * 3, 3)
    for h in range(2):
        zcopy[0, h, 0].wait_recv()
        zsend(1, h, 0, slot(xh, z - sign[h]))
    for copy in wq_mate:
        copy.wait_recv()
    project(own, (1 - c) * 3, 3)
    attend_all(own)

    wo_cross.wait_recv()
    for h in range(2):
        xsend(0, h, 1, own)
    rows = WO.at[part(far_seg, y)]
    wo_y = [send(rows, rows, wos.at[2 + k], wor.at[2 + k], ydev[k]) for k in range(3)]
    wo_fwd = [send(rows, rows, wos.at[5], wor.at[5], mate)]

    for h in range(2):
        zcopy[0, h, 1].wait_recv()
        zsend(1, h, 1, slot(xh, z - sign[h]))
    project_pair(xh, 0)
    for h in range(2):
        zcopy[1, h, 0].wait_recv()
        zsend(2, h, 0, slot(xh, z + 2))
        xsend(1, h, 0, slot(xh, z + 2))
    for h in range(2):
        zcopy[1, h, 1].wait_recv()
        xcopy[0, h].wait_recv()
        zsend(3, h, 1, slot(1 - xh, z))
        zsend(2, h, 1, slot(xh, z + 2))
    project(slot(xh, z + 2), 0, 6)
    attend_all(slot(xh, z + 2))

    load_g.wait()
    for copy in g_rs:
        copy.wait_recv()

    def sum4(rows):
        GX[rows, :] = (
            (GO[rows, :].astype(F32) + GR[0, rows, :].astype(F32))
            + (GR[1, rows, :].astype(F32) + GR[2, rows, :].astype(F32))
        ).astype(BF)
    by_rows(GROWS, sum4)
    g_half = [pl.ds(0, 16), pl.ds(16, GROWS - 16)]

    def g_swap(i):
        return send(GX.at[g_half[i]], GXR.at[g_half[i]], gs.at[3 + i], gr.at[3 + i], xlo)

    for h in range(2):
        xsend(2, h, 0, slot(xh, z - sign[h]))
    g_x = [g_swap(0)]

    for h in range(2):
        zcopy[3, h, 1].wait_recv()
        zsend(4, h, 1, slot(1 - xh, z - sign[h]))
    for h in range(2):
        xcopy[1, h].wait_recv()
        zsend(3, h, 0, slot(1 - xh, z + 2))
    for q in range(2):
        for h in range(2):
            zcopy[2, h, q].wait_recv()
    project_pair(xh, 1)
    attend_all(slot(xh, z + 1), 1)
    attend_all(slot(xh, z + 3), 2)

    for h in range(2):
        zcopy[4, h, 1].wait_recv()
        zsend(5, h, 1, slot(1 - xh, z + 2))
    project(slot(1 - xh, z + 2), 0, 6)
    attend_all(slot(1 - xh, z + 2))
    ctx_send(2)
    g_x.append(g_swap(1))

    for k in range(3):
        wo_y[k].wait_recv()
        rows = WO.at[part(far_seg, lax.rem(y + NY - k - 1, NY))]
        wo_fwd.append(send(rows, rows, wos.at[6 + k], wor.at[6 + k], mate))
    for h in range(2):
        xcopy[2, h].wait_recv()
    project_pair(1 - xh, 0)

    load_wo.wait()
    wo_mate.wait_recv()
    for copy in wo_fwd:
        copy.wait_recv()

    def out_tiles(fn):
        @pl.loop(0, D // 512)
        def _(j):
            fn(pl.ds(pl.multiple_of(j * 512, 512), 512))

    near = pl.ds(pl.multiple_of(xh * 2 * WIDTH, WIDTH), 2 * WIDTH)
    far = pl.ds(pl.multiple_of((1 - xh) * 2 * WIDTH, WIDTH), 2 * WIDTH)

    def out_rows(pieces):
        def joined(ref_at):
            parts = [ref_at(k, start, count) for k, start, count in pieces]
            return parts[0] if len(parts) == 1 else jnp.concatenate(parts, axis=0)

        def tile(cols):
            mine = joined(lambda k, start, count: CTX[slot(xh, z + k), start:start + count])
            theirs = joined(lambda k, start, count: CTXR[lax.rem(z + k, NZ), start:start + count])
            made = (
                jnp.dot(mine, WO[near, cols], preferred_element_type=F32)
                + jnp.dot(theirs, WO[far, cols], preferred_element_type=F32)
            ).astype(BF)
            at = 0
            for k, start, count in pieces:
                PS[lax.rem(z + k, NZ), start:start + count, cols] = made[at:at + count]
                at += count
        out_tiles(tile)

    ccopy[2, 0].wait_recv()
    out_rows([(2, 0, SEQ)])

    rcopy = {}

    def rsend(kind, q, image, h, to):
        ref = PS.at[lax.rem(image + 2 * NZ, NZ), quarter(h, q)]
        rcopy[kind, q] = send(
            ref, RB.at[kind, pl.ds(q * QUART, QUART)],
            rss.at[kind, q], rsr.at[kind, q], zdev[to],
        )

    for q in range(2):
        rsend(0, q, z + 2, 0, 1)
        rsend(1, q, z + 2, 1, 0)

    for h in range(2):
        zcopy[3, h, 0].wait_recv()
        zcopy[5, h, 1].wait_recv()
    project_pair(1 - xh, 1)
    for turn in range(2):
        halves = ((1, turn * HALF), (3, (1 - turn) * HALF))
        attention(*[(slot(1 - xh, z + k), (k + 1) // 2, start, HALF) for k, start in halves])
        for k, start in halves:
            ctx_send(k, start, HALF)
    for h in range(2):
        xsend(3, h, 0, own)

    for copy in g_x:
        copy.wait_recv()

    def sum2(rows):
        GT[rows, :] = (GX[rows, :].astype(F32) + GXR[rows, :].astype(F32)).astype(BF)
    by_rows(GROWS, sum2)
    g_ag = [send(GT, GA.at[k], gs.at[5 + k], gr.at[5 + k], ydev[k]) for k in range(3)]

    ccopy[1, 0].wait_recv()
    ccopy[3, HALF].wait_recv()
    out_rows([(1, 0, HALF), (3, HALF, HALF)])
    for q in range(2):
        rsend(4, q, z + 1, 0, 0)
        rsend(5, q, z - 1, 1, 1)
    ccopy[1, HALF].wait_recv()
    ccopy[3, 0].wait_recv()
    out_rows([(1, HALF, HALF), (3, 0, HALF)])

    for q in range(2):
        for h in range(2):
            image = lax.rem(z - sign[h] + NZ, NZ)
            rcopy[h, q].wait_recv()

            @pl.loop(0, QUART // 16)
            def _(i, h=h, q=q, image=image):
                at = pl.multiple_of(q * QUART + i * 16, 16)
                rows = pl.ds(h * HALF + at, 16)
                PS[image, rows, :] = (
                    PS[image, rows, :].astype(F32) + RB[h, pl.ds(at, 16), :].astype(F32)
                ).astype(BF)
            rsend(2 + h, q, z - sign[h], h, 1 - h)

    for h in range(2):
        xcopy[3, h].wait_recv()
    project(slot(1 - xh, z), 0, 6)
    attend_all(slot(1 - xh, z))
    ctx_send(0)
    ccopy[0, 0].wait_recv()
    out_rows([(0, 0, SEQ)])

    for copy in sent[:-9]:
        copy.wait_send()

    for k in range(4):
        if k:
            g_ag[k - 1].wait_recv()
        base = lax.rem(y + NY - k, NY) * GROWS

        def place(rows, k=k, base=base):
            part = GT[rows, :] if k == 0 else GA[k - 1, rows, :]
            gsum[pl.ds(pl.multiple_of(base + rows.start, 16), 16), :] = part.astype(F32)
        by_rows(GROWS, place)

    for q in range(2):
        for h in range(2):
            rcopy[4 + h, q].wait_recv()
            rcopy[2 + h, q].wait_recv()

            @pl.loop(0, QUART // 16)
            def _(i, h=h, q=q):
                at = pl.multiple_of(q * QUART + i * 16, 16)
                rows = pl.ds(h * HALF + at, 16)
                part = pl.ds(at, 16)
                proj = PS[z, rows, :].astype(F32) + (
                    RB[2 + h, part, :].astype(F32) + RB[4 + h, part, :].astype(F32)
                )
                OM[rows, :] = (raw[rows, :].astype(F32) + proj).astype(BF)
    for copy in sent[-9:]:
        copy.wait_send()


def finish(mixed_in, grad_in, mixed_out, grad_out, sem):
    made = [pltpu.make_async_copy(mixed_in, mixed_out, sem.at[4])]
    for i in range(4):
        rows = pl.ds(i * GROWS, GROWS)
        made.append(pltpu.make_async_copy(grad_in.at[rows], grad_out.at[rows], sem.at[i]))
    for copy in made:
        copy.start()
    for copy in made:
        copy.wait()


def body(tokens, ln_gain, ln_bias, w_qkv, w_out, grad_partial):
    dma = pltpu.SemaphoreType.DMA
    any_spec = pl.BlockSpec(memory_space=pl.ANY)
    vmem = pl.BlockSpec(memory_space=pltpu.VMEM)
    mixed, grad_sum = pl.pallas_call(
        kernel,
        out_shape=(pltpu.VMEM((SEQ, D), BF), pltpu.VMEM((WIDTH, D), F32)),
        in_specs=[any_spec, vmem, vmem, any_spec, any_spec, any_spec],
        out_specs=(vmem, vmem),
        scratch_shapes=[
            pltpu.VMEM((SEQ, D), BF),
            pltpu.VMEM((2 * NZ, SEQ, D), BF),
            pltpu.VMEM((6, D, WIDTH), BF),
            pltpu.VMEM((4 * WIDTH, D), BF),
            pltpu.VMEM((3, 6, SEQ, WIDTH), BF),
            pltpu.VMEM((2 * NZ, SEQ, 2 * WIDTH), BF),
            pltpu.VMEM((NZ, SEQ, 2 * WIDTH), BF),
            pltpu.VMEM((NZ, SEQ, D), BF),
            pltpu.VMEM((6, HALF, D), BF),
            pltpu.VMEM((GROWS, D), BF),
            pltpu.VMEM((3, GROWS, D), BF),
            pltpu.VMEM((GROWS, D), BF),
            pltpu.VMEM((GROWS, D), BF),
            pltpu.VMEM((GROWS, D), BF),
            pltpu.VMEM((3, GROWS, D), BF),
            dma((6, 2, 2)), dma((6, 2, 2)),
            dma((4, 2)), dma((4, 2)),
            dma((4, 2)), dma((4, 2)),
            dma((6, 2)), dma((6, 2)),
            dma((3,)), dma((3,)),
            dma((9,)), dma((9,)),
            dma((8,)), dma((8,)),
            dma((10,)),
        ],
        compiler_params=pltpu.CompilerParams(
            collective_id=0, has_side_effects=True, vmem_limit_bytes=57671680
        ),
    )(
        tokens[0], ln_gain[None], ln_bias[None],
        jnp.transpose(w_qkv, (1, 0, 2)), w_out, grad_partial[0],
    )
    mixed = pltpu.with_memory_space_constraint(mixed, pltpu.VMEM)
    grad_sum = pltpu.with_memory_space_constraint(grad_sum, pltpu.VMEM)
    mixed, grad_sum = pl.pallas_call(
        finish,
        out_shape=(
            jax.ShapeDtypeStruct((SEQ, D), BF),
            jax.ShapeDtypeStruct((WIDTH, D), F32),
        ),
        in_specs=[vmem, vmem],
        out_specs=(any_spec, any_spec),
        scratch_shapes=[dma((5,))],
        compiler_params=pltpu.CompilerParams(vmem_limit_bytes=1 << 20),
    )(mixed, grad_sum)
    return (mixed[None], grad_sum)


def solution(mesh):
    placed = (
        P("dp", "mp", None),
        P(),
        P(),
        P(None, None, "mp"),
        P("mp", None),
        P("dp", "mp", None),
    )
    return jax.shard_map(
        body,
        mesh=mesh,
        in_specs=placed,
        out_specs=(P("dp", "mp", None), P("mp", None)),
        check_vma=False,
    )
```

```python
import jax
import jax.numpy as jnp
from jax import lax
from jax.experimental import pallas as pl
from jax.experimental.pallas import tpu as pltpu
from jax.sharding import PartitionSpec as P

HEAD = 128
SEQ = 128
D = 5120
NY = 4
NZ = 4
WIDTH = 256
HALF = SEQ // 2
QUART = SEQ // 4
GROWS = WIDTH // NY
MESH = pl.DeviceIdType.MESH
BF = jnp.bfloat16
F32 = jnp.float32


def attend(heads):
    scores = [
        lax.dot_general(query, keys, (((1,), (1,)), ((), ())), preferred_element_type=F32)
        * HEAD ** (-0.5)
        for query, keys, _ in heads
    ]
    tops = [jnp.max(part, axis=-1, keepdims=True) for part in scores]
    expsc = [jnp.exp(part - top) for part, top in zip(scores, tops)]
    sums = [jnp.sum(part, axis=-1, keepdims=True) for part in expsc]
    attn = [(part / total).astype(BF) for part, total in zip(expsc, sums)]
    return [
        jnp.dot(part, values, preferred_element_type=F32).astype(BF)
        for part, (_, _, values) in zip(attn, heads)
    ]


def kernel(
    tok_hbm, gain, bias, wq_hbm, wo_hbm, g_hbm,
    OM, gsum,
    raw, T, WQ, WO, QKV, CTX, CTXR, PS, RB,
    GO, GR, GX, GXR, GT, GA,
    zs, zr, xs, xr, cs, cr, rss, rsr,
    wqs, wqr, wos, wor, gs, gr, loc,
):
    dp = lax.axis_index("dp")
    mp = lax.axis_index("mp")
    y, xl = dp // 2, dp % 2
    xh, z, c = mp // 8, (mp // 2) % 4, mp % 2

    def dev(y, xl, xh, z, c):
        return (lax.rem(y + NY, NY) * 2 + xl, xh * 8 + lax.rem(z + NZ, NZ) * 2 + c)

    zdev = (dev(y, xl, xh, z + 1, c), dev(y, xl, xh, z - 1, c))
    x2 = dev(y, xl, 1 - xh, z, c)
    mate = dev(y, xl, xh, z, 1 - c)
    cross = dev(y, 1 - xl, 1 - xh, z, c)
    xlo = dev(y, 1 - xl, xh, z, c)
    ydev = [dev(y + k, xl, xh, z, c) for k in (1, 2, 3 - NY)]

    barrier = pltpu.get_barrier_semaphore()
    peers = [*zdev, x2, mate, cross, xlo, *ydev]
    for peer in peers:
        pl.semaphore_signal(barrier, inc=1, device_id=peer, device_id_type=MESH)

    def local(src, dst, sem):
        copy = pltpu.make_async_copy(src, dst, sem)
        copy.start()
        return copy

    def quarter(h, q):
        return pl.ds(h * HALF + q * QUART, QUART)

    load_raw = [
        [local(tok_hbm.at[quarter(h, q)], raw.at[quarter(h, q)], loc.at[6 + 2 * q + h]) for h in range(2)]
        for q in range(2)
    ]
    load_wq = [local(wq_hbm.at[j], WQ.at[c * 3 + j], loc.at[1 + j]) for j in range(3)]
    own_seg = pl.multiple_of((xh * 2 + c) * WIDTH, WIDTH)
    far_seg = pl.multiple_of(((1 - xh) * 2 + c) * WIDTH, WIDTH)
    load_wo = local(wo_hbm, WO.at[pl.ds(own_seg, WIDTH)], loc.at[4])
    my_rows = pl.ds(pl.multiple_of(y * GROWS, GROWS), GROWS)
    load_g = local(g_hbm.at[my_rows], GO, loc.at[5])

    def slot(col, zz):
        return col * NZ + lax.rem(zz + 2 * NZ, NZ)

    own = slot(xh, z)
    def norm_rows(h, q):
        load_raw[q][h].wait()

        @pl.loop(0, QUART // 16)
        def _(i):
            rows = pl.ds(pl.multiple_of(h * HALF + q * QUART + i * 16, 16), 16)
            values = raw[rows, :].astype(F32)
            center = jnp.mean(values, axis=-1, keepdims=True)
            spread = jnp.mean((values - center) * (values - center), axis=-1, keepdims=True)
            T[own, rows, :] = (
                (values - center) * lax.rsqrt(spread + 1e-06) * gain[...] + bias[...]
            ).astype(BF)

    for h in range(2):
        norm_rows(h, 0)
    pl.semaphore_wait(barrier, len(peers))

    sent = []

    def send(src, dst, ssem, rsem, peer):
        copy = pltpu.make_async_remote_copy(
            src_ref=src, dst_ref=dst, send_sem=ssem, recv_sem=rsem,
            device_id=peer, device_id_type=MESH,
        )
        copy.start()
        sent.append(copy)
        return copy

    def part(seg, yy):
        return pl.ds(pl.multiple_of(seg + yy * GROWS, GROWS), GROWS)

    wo_cross = send(
        wo_hbm.at[part(0, y)], WO.at[part(own_seg, y)], wos.at[0], wor.at[0], cross
    )

    zcopy, xcopy = {}, {}

    def zsend(step, h, q, s):
        ref = T.at[s, quarter(h, q)]
        zcopy[step, h, q] = send(ref, ref, zs.at[step, h, q], zr.at[step, h, q], zdev[h])

    def xsend(step, h, q, s):
        ref = T.at[s, quarter(h, q)]
        xcopy[step, h] = send(ref, ref, xs.at[step, h], xr.at[step, h], x2)

    sign = (1, -1)
    for h in range(2):
        zsend(0, h, 0, own)
    wq_mate = [
        send(wq_hbm.at[j], WQ.at[c * 3 + j], wqs.at[j], wqr.at[j], mate) for j in range(3)
    ]
    wo_mate = send(wo_hbm, WO.at[pl.ds(own_seg, WIDTH)], wos.at[1], wor.at[1], mate)
    g_rs = []
    for k in range(3):
        rows = pl.ds(pl.multiple_of(lax.rem(y + k + 1, NY) * GROWS, GROWS), GROWS)
        g_rs.append(send(g_hbm.at[rows], GR.at[k], gs.at[k], gr.at[k], ydev[k]))

    def project(s, base, count):
        @pl.loop(0, count)
        def _(j):
            QKV[0, base + j] = jnp.dot(T[s], WQ[base + j], preferred_element_type=F32).astype(BF)

    def project_pair(col, way):
        up, down = slot(col, z + 1), slot(col, z + 3)
        at_up, at_down = (1 - way) * HALF, way * HALF

        @pl.loop(0, 6)
        def _(j):
            lhs = jnp.concatenate(
                [T[up, at_up:at_up + HALF], T[down, at_down:at_down + HALF]], axis=0
            )
            both = jnp.dot(lhs, WQ[j], preferred_element_type=F32).astype(BF)
            QKV[1, j, at_up:at_up + HALF] = both[:HALF]
            QKV[2, j, at_down:at_down + HALF] = both[HALF:]

    def attention(*units):
        heads, places = [], []
        for s, b, start, count in units:
            rows = slice(start, start + count)
            for cc in range(2):
                for h in range(2):
                    cols = slice(h * HEAD, (h + 1) * HEAD)
                    heads.append((
                        QKV[b, cc * 3, rows, cols], QKV[b, cc * 3 + 1, :, cols],
                        QKV[b, cc * 3 + 2, :, cols],
                    ))
                    at = cc * WIDTH + h * HEAD
                    places.append((s, rows, slice(at, at + HEAD)))
        for place, made in zip(places, attend(heads)):
            CTX[place] = made

    def attend_all(s, b=0):
        attention((s, b, 0, SEQ))

    ccopy = {}

    def ctx_send(k, start=0, count=SEQ):
        rows = pl.ds(start, count)
        sems = (cs.at[k, start // HALF], cr.at[k, start // HALF])
        ccopy[k, start] = send(
            CTX.at[slot(1 - xh, z + k), rows], CTXR.at[lax.rem(z + k, NZ), rows], *sems, x2
        )

    for h in range(2):
        norm_rows(h, 1)
        zsend(0, h, 1, own)

    def by_rows(count, fn):
        @pl.loop(0, count // 16)
        def _(i):
            fn(pl.ds(pl.multiple_of(i * 16, 16), 16))

    for copy in load_wq:
        copy.wait()
    project(own, c * 3, 3)
    for h in range(2):
        zcopy[0, h, 0].wait_recv()
        zsend(1, h, 0, slot(xh, z - sign[h]))
    for copy in wq_mate:
        copy.wait_recv()
    project(own, (1 - c) * 3, 3)
    attend_all(own)

    wo_cross.wait_recv()
    for h in range(2):
        xsend(0, h, 1, own)
    rows = WO.at[part(far_seg, y)]
    wo_y = [send(rows, rows, wos.at[2 + k], wor.at[2 + k], ydev[k]) for k in range(3)]
    wo_fwd = [send(rows, rows, wos.at[5], wor.at[5], mate)]

    for h in range(2):
        zcopy[0, h, 1].wait_recv()
        zsend(1, h, 1, slot(xh, z - sign[h]))
    project_pair(xh, 0)
    for h in range(2):
        zcopy[1, h, 0].wait_recv()
        zsend(2, h, 0, slot(xh, z + 2))
        xsend(1, h, 0, slot(xh, z + 2))
    for h in range(2):
        zcopy[1, h, 1].wait_recv()
        xcopy[0, h].wait_recv()
        zsend(3, h, 1, slot(1 - xh, z))
        zsend(2, h, 1, slot(xh, z + 2))
    project(slot(xh, z + 2), 0, 6)
    attend_all(slot(xh, z + 2))

    load_g.wait()
    for copy in g_rs:
        copy.wait_recv()

    def sum4(rows):
        GX[rows, :] = (
            (GO[rows, :].astype(F32) + GR[0, rows, :].astype(F32))
            + (GR[1, rows, :].astype(F32) + GR[2, rows, :].astype(F32))
        ).astype(BF)
    by_rows(GROWS, sum4)
    g_half = [pl.ds(0, 48), pl.ds(48, GROWS - 48)]

    def g_swap(i):
        return send(GX.at[g_half[i]], GXR.at[g_half[i]], gs.at[3 + i], gr.at[3 + i], xlo)

    for h in range(2):
        xsend(2, h, 0, slot(xh, z - sign[h]))

    for h in range(2):
        zcopy[3, h, 1].wait_recv()
        zsend(4, h, 1, slot(1 - xh, z - sign[h]))
    for h in range(2):
        xcopy[1, h].wait_recv()
        zsend(3, h, 0, slot(1 - xh, z + 2))
    for q in range(2):
        for h in range(2):
            zcopy[2, h, q].wait_recv()
    project_pair(xh, 1)
    attend_all(slot(xh, z + 1), 1)
    attend_all(slot(xh, z + 3), 2)

    for h in range(2):
        zcopy[4, h, 1].wait_recv()
        zsend(5, h, 1, slot(1 - xh, z + 2))
    project(slot(1 - xh, z + 2), 0, 6)
    attend_all(slot(1 - xh, z + 2))
    ctx_send(2)
    g_x = [g_swap(0)]

    for k in range(3):
        wo_y[k].wait_recv()
        rows = WO.at[part(far_seg, lax.rem(y + NY - k - 1, NY))]
        wo_fwd.append(send(rows, rows, wos.at[6 + k], wor.at[6 + k], mate))
    for h in range(2):
        xcopy[2, h].wait_recv()
    project_pair(1 - xh, 0)

    load_wo.wait()
    wo_mate.wait_recv()
    for copy in wo_fwd:
        copy.wait_recv()

    def out_tiles(fn):
        @pl.loop(0, D // 512)
        def _(j):
            fn(pl.ds(pl.multiple_of(j * 512, 512), 512))

    near = pl.ds(pl.multiple_of(xh * 2 * WIDTH, WIDTH), 2 * WIDTH)
    far = pl.ds(pl.multiple_of((1 - xh) * 2 * WIDTH, WIDTH), 2 * WIDTH)

    def out_rows(pieces):
        def joined(ref_at):
            parts = [ref_at(k, start, count) for k, start, count in pieces]
            return parts[0] if len(parts) == 1 else jnp.concatenate(parts, axis=0)

        def tile(cols):
            mine = joined(lambda k, start, count: CTX[slot(xh, z + k), start:start + count])
            theirs = joined(lambda k, start, count: CTXR[lax.rem(z + k, NZ), start:start + count])
            made = (
                jnp.dot(mine, WO[near, cols], preferred_element_type=F32)
                + jnp.dot(theirs, WO[far, cols], preferred_element_type=F32)
            ).astype(BF)
            at = 0
            for k, start, count in pieces:
                PS[lax.rem(z + k, NZ), start:start + count, cols] = made[at:at + count]
                at += count
        out_tiles(tile)

    ccopy[2, 0].wait_recv()
    out_rows([(2, 0, SEQ)])

    rcopy = {}

    def rsend(kind, q, image, h, to):
        ref = PS.at[lax.rem(image + 2 * NZ, NZ), quarter(h, q)]
        rcopy[kind, q] = send(
            ref, RB.at[kind, pl.ds(q * QUART, QUART)],
            rss.at[kind, q], rsr.at[kind, q], zdev[to],
        )

    for q in range(2):
        rsend(0, q, z + 2, 0, 1)
        rsend(1, q, z + 2, 1, 0)

    for h in range(2):
        zcopy[3, h, 0].wait_recv()
        zcopy[5, h, 1].wait_recv()
    project_pair(1 - xh, 1)
    for turn in range(2):
        halves = ((1, turn * HALF), (3, (1 - turn) * HALF))
        attention(*[(slot(1 - xh, z + k), (k + 1) // 2, start, HALF) for k, start in halves])
        for k, start in halves:
            ctx_send(k, start, HALF)
    for h in range(2):
        xsend(3, h, 0, own)
    g_x.append(g_swap(1))

    g_ag = []

    def g_share(i):
        g_x[i].wait_recv()

        @pl.loop(0, g_half[i].size // 16)
        def _(j):
            rows = pl.ds(pl.multiple_of(g_half[i].start + j * 16, 16), 16)
            GT[rows, :] = (GX[rows, :].astype(F32) + GXR[rows, :].astype(F32)).astype(BF)
        for k in range(3):
            g_ag.append(send(
                GT.at[g_half[i]], GA.at[k, g_half[i]],
                gs.at[5 + 3 * i + k], gr.at[5 + 3 * i + k], ydev[k],
            ))

    g_share(0)
    ccopy[1, 0].wait_recv()
    ccopy[3, HALF].wait_recv()
    out_rows([(1, 0, HALF), (3, HALF, HALF)])
    for q in range(2):
        rsend(4, q, z + 1, 0, 0)
        rsend(5, q, z - 1, 1, 1)
    ccopy[1, HALF].wait_recv()
    ccopy[3, 0].wait_recv()
    out_rows([(1, HALF, HALF), (3, 0, HALF)])

    for q in range(2):
        for h in range(2):
            image = lax.rem(z - sign[h] + NZ, NZ)
            rcopy[h, q].wait_recv()

            @pl.loop(0, QUART // 16)
            def _(i, h=h, q=q, image=image):
                at = pl.multiple_of(q * QUART + i * 16, 16)
                rows = pl.ds(h * HALF + at, 16)
                PS[image, rows, :] = (
                    PS[image, rows, :].astype(F32) + RB[h, pl.ds(at, 16), :].astype(F32)
                ).astype(BF)
            rsend(2 + h, q, z - sign[h], h, 1 - h)

    for h in range(2):
        xcopy[3, h].wait_recv()
    project(slot(1 - xh, z), 0, 6)
    attend_all(slot(1 - xh, z))
    ctx_send(0)
    g_share(1)
    ccopy[0, 0].wait_recv()
    out_rows([(0, 0, SEQ)])

    for copy in sent[:-12]:
        copy.wait_send()

    for k in range(4):
        if k:
            g_ag[k - 1].wait_recv()
            g_ag[k + 2].wait_recv()
        base = lax.rem(y + NY - k, NY) * GROWS

        def place(rows, k=k, base=base):
            part = GT[rows, :] if k == 0 else GA[k - 1, rows, :]
            gsum[pl.ds(pl.multiple_of(base + rows.start, 16), 16), :] = part.astype(F32)
        by_rows(GROWS, place)

    for q in range(2):
        for h in range(2):
            rcopy[4 + h, q].wait_recv()
            rcopy[2 + h, q].wait_recv()

            @pl.loop(0, QUART // 16)
            def _(i, h=h, q=q):
                at = pl.multiple_of(q * QUART + i * 16, 16)
                rows = pl.ds(h * HALF + at, 16)
                part = pl.ds(at, 16)
                proj = PS[z, rows, :].astype(F32) + (
                    RB[2 + h, part, :].astype(F32) + RB[4 + h, part, :].astype(F32)
                )
                OM[rows, :] = (raw[rows, :].astype(F32) + proj).astype(BF)
    for copy in sent[-12:]:
        copy.wait_send()


def finish(mixed_in, grad_in, mixed_out, grad_out, sem):
    made = [pltpu.make_async_copy(mixed_in, mixed_out, sem.at[4])]
    for i in range(4):
        rows = pl.ds(i * GROWS, GROWS)
        made.append(pltpu.make_async_copy(grad_in.at[rows], grad_out.at[rows], sem.at[i]))
    for copy in made:
        copy.start()
    for copy in made:
        copy.wait()


def body(tokens, ln_gain, ln_bias, w_qkv, w_out, grad_partial):
    dma = pltpu.SemaphoreType.DMA
    any_spec = pl.BlockSpec(memory_space=pl.ANY)
    vmem = pl.BlockSpec(memory_space=pltpu.VMEM)
    mixed, grad_sum = pl.pallas_call(
        kernel,
        out_shape=(pltpu.VMEM((SEQ, D), BF), pltpu.VMEM((WIDTH, D), F32)),
        in_specs=[any_spec, vmem, vmem, any_spec, any_spec, any_spec],
        out_specs=(vmem, vmem),
        scratch_shapes=[
            pltpu.VMEM((SEQ, D), BF),
            pltpu.VMEM((2 * NZ, SEQ, D), BF),
            pltpu.VMEM((6, D, WIDTH), BF),
            pltpu.VMEM((4 * WIDTH, D), BF),
            pltpu.VMEM((3, 6, SEQ, WIDTH), BF),
            pltpu.VMEM((2 * NZ, SEQ, 2 * WIDTH), BF),
            pltpu.VMEM((NZ, SEQ, 2 * WIDTH), BF),
            pltpu.VMEM((NZ, SEQ, D), BF),
            pltpu.VMEM((6, HALF, D), BF),
            pltpu.VMEM((GROWS, D), BF),
            pltpu.VMEM((3, GROWS, D), BF),
            pltpu.VMEM((GROWS, D), BF),
            pltpu.VMEM((GROWS, D), BF),
            pltpu.VMEM((GROWS, D), BF),
            pltpu.VMEM((3, GROWS, D), BF),
            dma((6, 2, 2)), dma((6, 2, 2)),
            dma((4, 2)), dma((4, 2)),
            dma((4, 2)), dma((4, 2)),
            dma((6, 2)), dma((6, 2)),
            dma((3,)), dma((3,)),
            dma((9,)), dma((9,)),
            dma((11,)), dma((11,)),
            dma((10,)),
        ],
        compiler_params=pltpu.CompilerParams(
            collective_id=0, has_side_effects=True, vmem_limit_bytes=57671680
        ),
    )(
        tokens[0], ln_gain[None], ln_bias[None],
        jnp.transpose(w_qkv, (1, 0, 2)), w_out, grad_partial[0],
    )
    mixed = pltpu.with_memory_space_constraint(mixed, pltpu.VMEM)
    grad_sum = pltpu.with_memory_space_constraint(grad_sum, pltpu.VMEM)
    mixed, grad_sum = pl.pallas_call(
        finish,
        out_shape=(
            jax.ShapeDtypeStruct((SEQ, D), BF),
            jax.ShapeDtypeStruct((WIDTH, D), F32),
        ),
        in_specs=[vmem, vmem],
        out_specs=(any_spec, any_spec),
        scratch_shapes=[dma((5,))],
        compiler_params=pltpu.CompilerParams(vmem_limit_bytes=1 << 20),
    )(mixed, grad_sum)
    return (mixed[None], grad_sum)


def solution(mesh):
    placed = (
        P("dp", "mp", None),
        P(),
        P(),
        P(None, None, "mp"),
        P("mp", None),
        P("dp", "mp", None),
    )
    return jax.shard_map(
        body,
        mesh=mesh,
        in_specs=placed,
        out_specs=(P("dp", "mp", None), P("mp", None)),
        check_vma=False,
    )
```
